32 devices in a mesh: parts: 2 (over y), gz: 4 (over z), shot: 4 (over x, core).
Axes of the slice: x: 2, y: 2, z: 4, core: 2. Of those that a mesh axis runs over, the one named last changes fastest.
Arguments:
- wavefields: float32 [8, 2, 9, 16, 32, 128], P(('parts', 'shot'), None, None, 'gz'), parts along dimension 0, may hold values from -6 to 6
- earth_model: float32 [6, 16, 32, 128], P('parts', 'gz'), parts along dimension 0, may hold values from 0.4 to 1.6
- source_depth: int32 [8], P(('parts', 'shot')), parts along dimension 0, may hold values from 0 to 15
- source_column: int32 [8], P(('parts', 'shot')), parts along dimension 0, may hold values from 0 to 4095
- wavelet: float32 [8, 8], P(('parts', 'shot')), parts along dimension 0, may hold values from -30 to 30
- receiver_depth: int32 [8, 64], P(('parts', 'shot')), parts along dimension 0, may hold values from 0 to 15
- receiver_column: int32 [8, 64], P(('parts', 'shot')), parts along dimension 0, may hold values from 0 to 4095
- traces: float32 [8, 8, 64], P(('parts', 'shot')), parts along dimension 0, may hold values from -30 to 30
Outputs:
- images: float32 [4, 16, 32, 128], P('parts', 'gz'), parts along dimension 0
The draws below stay inside these ranges and needn't reach their ends.
There are 2 independent parts, one for each index of `parts`. The reference program is written for one: setup_inputs(seed, part) draws one part's arguments, and reference() takes and returns one part's arrays. A program takes and returns all parts, laid end to end along the dimension named above; each array names one. Nothing has to cross between parts.
All inputs are finite; a program needn't handle non-finite values.
Results may differ from the reference program's by a relative error of at most 0.00002.
Values sent between devices are 32-bit elements; how exact they have to be, the bound alone decides.
A program may use at most 64 MiB of HBM per device.

```python
import math
import jax
import jax.numpy as jnp
from jax import lax

NX = 32
NY = 128
STEPS = 8
RECV = 64
NZ = 16
SHOTS = 4


def plant(drawn, key, smallest, top_value):
    dims = drawn.shape
    spot = [jax.random.randint(jax.random.fold_in(key, axis), (), 0, dims[axis]) for axis in range(len(dims))]
    drawn = drawn.at[tuple(spot)].set(smallest)
    longest = dims.index(max(dims))
    spot[longest] = (spot[longest] + 1) % dims[longest]
    return drawn.at[tuple(spot)].set(top_value)


def levels(stream_key, extent, pieces, least, top_value):
    loudness = 1.0
    for position, parts in pieces:
        heights = jax.random.uniform(jax.random.fold_in(jax.random.fold_in(stream_key, 6), position), (parts,), jnp.float32, least / len(pieces), top_value / len(pieces))
        loudness = loudness * jnp.repeat(jnp.exp(heights), extent[position] // parts).reshape((-1,) + (1,) * (len(extent) - 1 - position))
    return loudness


def noise(stream_key, shape, scale, most, cuts=(), held_as=jnp.bfloat16):
    result = scale * jax.random.normal(stream_key, shape, jnp.float32)
    if cuts:
        result = result * levels(stream_key, shape, cuts, -0.22, 0.18)
    return jnp.clip(result, -most, most).astype(held_as)


def setup_inputs(seed: int = 0, part: int = 0) -> dict:
    key_list = jax.random.split(jax.random.key(seed), 9)
    part_keys = jax.random.split(jax.random.fold_in(key_list[8], part), 9)
    return {
        "wavefields": noise(part_keys[0], (SHOTS, 2, 9, NZ, NX, NY), 1.0, 6.0, ((0, 4), (3, 4)), jnp.float32),
        "earth_model": jnp.clip(jnp.exp(math.log(1.6) - 1.3862944 * jax.random.uniform(part_keys[1], (3, NZ, NX, NY), jnp.float32) ** levels(part_keys[1], (3, NZ, NX, NY), ((1, 4),), -0.2, 0.2)), 0.4, 1.6),
        "source_depth": plant(jax.random.randint(part_keys[2], (SHOTS,), 0, NZ), jax.random.fold_in(part_keys[2], 1), 0, NZ - 1).astype(jnp.int32),
        "source_column": plant(jax.random.randint(part_keys[3], (SHOTS,), 0, NX * NY), jax.random.fold_in(part_keys[3], 1), 0, (NX * NY) - 1).astype(jnp.int32),
        "wavelet": noise(part_keys[4], (SHOTS, STEPS), 5.0, 30.0, ((0, 4),), jnp.float32),
        "receiver_depth": plant(jax.random.randint(part_keys[5], (SHOTS, RECV), 0, NZ), jax.random.fold_in(part_keys[5], 1), 0, NZ - 1).astype(jnp.int32),
        "receiver_column": plant(jax.random.randint(part_keys[6], (SHOTS, RECV), 0, NX * NY), jax.random.fold_in(part_keys[6], 1), 0, (NX * NY) - 1).astype(jnp.int32),
        "traces": noise(part_keys[7], (SHOTS, STEPS, RECV), 5.0, 30.0, ((0, 4),), jnp.float32),
    }


time_step = 0.15


def forward_diff(array, dim_index):
    length = array.shape[dim_index]
    following = jnp.concatenate([lax.slice_in_dim(array, 1, length, axis=dim_index), jnp.zeros_like(lax.slice_in_dim(array, 0, 1, axis=dim_index))], axis=dim_index)
    return following - array


def backward_diff(array, dim_index):
    length = array.shape[dim_index]
    previous = jnp.concatenate([jnp.zeros_like(lax.slice_in_dim(array, 0, 1, axis=dim_index)), lax.slice_in_dim(array, 0, length - 1, axis=dim_index)], axis=dim_index)
    return array - previous


def depth_forward(array, plane_high):
    following = jnp.concatenate([array[:, 1:], plane_high[:, None]], axis=1)
    return following - array


def depth_backward(array, plane_low):
    previous = jnp.concatenate([plane_low[:, None], array[:, :-1]], axis=1)
    return array - previous


def velocity_half(fields, buoyancy, sxz_low, syz_low, szz_high):
    vel_x, vel_y, vel_z, sig_xx, sig_yy, sig_zz, sig_xy, sig_xz, sig_yz = fields
    vel_x = vel_x + time_step * buoyancy * (forward_diff(sig_xx, 2) + backward_diff(sig_xy, 3) + depth_backward(sig_xz, sxz_low))
    vel_y = vel_y + time_step * buoyancy * (backward_diff(sig_xy, 2) + forward_diff(sig_yy, 3) + depth_backward(sig_yz, syz_low))
    vel_z = vel_z + time_step * buoyancy * (backward_diff(sig_xz, 2) + backward_diff(sig_yz, 3) + depth_forward(sig_zz, szz_high))
    return vel_x, vel_y, vel_z


def stress_half(fields, lame_lambda, shear_mu, vz_low, vx_high, vy_high):
    vel_x, vel_y, vel_z, sig_xx, sig_yy, sig_zz, sig_xy, sig_xz, sig_yz = fields
    strain_x = backward_diff(vel_x, 2)
    strain_y = backward_diff(vel_y, 3)
    strain_z = depth_backward(vel_z, vz_low)
    spread = strain_x + strain_y + strain_z
    sig_xx = sig_xx + time_step * (lame_lambda * spread + 2.0 * shear_mu * strain_x)
    sig_yy = sig_yy + time_step * (lame_lambda * spread + 2.0 * shear_mu * strain_y)
    sig_zz = sig_zz + time_step * (lame_lambda * spread + 2.0 * shear_mu * strain_z)
    vx_up = depth_forward(vel_x, vx_high)
    vy_up = depth_forward(vel_y, vy_high)
    vz_along_x = forward_diff(vel_z, 2)
    vz_along_y = forward_diff(vel_z, 3)
    vx_along_y = forward_diff(vel_x, 3)
    vy_along_x = forward_diff(vel_y, 2)
    sig_xy = sig_xy + time_step * shear_mu * (vx_along_y + vy_along_x)
    sig_xz = sig_xz + time_step * shear_mu * (vx_up + vz_along_x)
    sig_yz = sig_yz + time_step * shear_mu * (vy_up + vz_along_y)
    rotation = (vz_along_y - vy_up) + (vx_up - vz_along_x) + (vy_along_x - vx_along_y)
    return [vel_x, vel_y, vel_z, sig_xx, sig_yy, sig_zz, sig_xy, sig_xz, sig_yz], rotation


def reference(wavefields, earth_model, source_depth, source_column, wavelet, receiver_depth, receiver_column, traces):
    buoyancy = earth_model[0]
    lame_lambda = earth_model[1]
    shear_mu = earth_model[2]
    image_pp = jnp.zeros((NZ, NX, NY), jnp.float32)
    image_ps = jnp.zeros((NZ, NX, NY), jnp.float32)
    zero_plane = jnp.zeros((2, NX, NY), jnp.float32)
    for shot_index in range(SHOTS):
        fields = [wavefields[shot_index, :, field_no] for field_no in range(9)]
        src_row = source_column[shot_index] // NY
        src_col = source_column[shot_index] % NY
        rec_row = receiver_column[shot_index] // NY
        rec_col = receiver_column[shot_index] % NY
        for step_index in range(STEPS):
            vel_x, vel_y, vel_z = velocity_half(fields, buoyancy, zero_plane, zero_plane, zero_plane)
            vel_z = vel_z.at[1, receiver_depth[shot_index], rec_row, rec_col].add(time_step * traces[shot_index, step_index])
            fields, rotation = stress_half([vel_x, vel_y, vel_z] + list(fields[3:]), lame_lambda, shear_mu, zero_plane, zero_plane, zero_plane)
            for field_no in (3, 4, 5):
                fields[field_no] = fields[field_no].at[0, source_depth[shot_index], src_row, src_col].add(time_step * wavelet[shot_index, step_index])
            pressure = (fields[3] + fields[4] + fields[5]) / 3.0
            image_pp = image_pp + pressure[0] * pressure[1]
            image_ps = image_ps + pressure[0] * rotation[1]
    return jnp.stack([image_pp, image_ps]) / STEPS
```

```python
import functools

import jax
import jax.numpy as jnp
from jax import lax
from jax.experimental import pallas as pl
from jax.experimental.pallas import tpu as pltpu
from jax.sharding import PartitionSpec as P

time_step = 0.15
VX, VY, VZ, SXX, SYY, SZZ, SXY, SXZ, SYZ = range(9)
MESH = pl.DeviceIdType.MESH


def kernel(
    gz_count,
    shot_count,
    wave_hbm,
    earth_hbm,
    src_depth_hbm,
    src_column_hbm,
    wavelet_hbm,
    rec_depth_hbm,
    rec_column_hbm,
    traces_hbm,
    out,
    state,
    earth,
    below,
    below_earth,
    above,
    above_earth,
    first_up,
    first_szz,
    earth_up,
    earth_down,
    low_in,
    high_in,
    up_out,
    down_out,
    rest_in,
    rest_out,
    inject,
    press,
    spin,
    image,
    parts_in,
    own,
    src_depth,
    src_column,
    wavelet,
    rec_depth,
    rec_column,
    traces,
    load_sem,
    init_send,
    init_recv,
    up_send,
    up_recv,
    down_send,
    down_recv,
    rest_sem,
    img_send,
    img_recv,
):
    planes, nx, ny = state.shape[2:]
    steps = traces.shape[0]
    last = planes - 1
    h = time_step
    gz = lax.axis_index("gz")
    shot = lax.axis_index("shot")
    has_low = gz > 0
    has_high = gz < gz_count - 1
    paired = shot_count % 2 == 0
    far = lax.rem(shot, 2) == 0

    def local(src, dst, k):
        return pltpu.make_async_copy(src, dst, load_sem.at[k])

    load_first = [
        [
            local(wave_hbm.at[0, w, pl.ds(SXZ, 2), last], first_up.at[w, pl.ds(0, 2)], 4 * w),
            local(wave_hbm.at[0, w, SZZ, 0], first_szz.at[w], 4 * w + 1),
            local(wave_hbm.at[0, w], state.at[w], 4 * w + 2),
        ]
        for w in range(2)
    ]
    load_edge = [
        local(earth_hbm.at[0, last], earth_up.at[0], 8),
        local(earth_hbm.at[2, last], earth_up.at[1], 9),
        local(earth_hbm.at[:, 0], earth_down, 10),
    ]
    load_earth = local(earth_hbm, earth, 11)
    small = [
        local(src, dst, 12 + i)
        for i, (src, dst) in enumerate(
            (
                (traces_hbm.at[0], traces),
                (rec_depth_hbm, rec_depth),
                (rec_column_hbm, rec_column),
                (src_depth_hbm, src_depth),
                (src_column_hbm, src_column),
                (wavelet_hbm, wavelet),
            )
        )
    ]
    for copy in load_edge[:1] + load_first[0] + load_first[1] + load_edge[1:] + [load_earth] + small:
        copy.start()

    barrier = pltpu.get_barrier_semaphore()

    @pl.when(has_low)
    def _():
        pl.semaphore_signal(barrier, inc=1, device_id={"gz": gz - 1}, device_id_type=MESH)

    @pl.when(has_high)
    def _():
        pl.semaphore_signal(barrier, inc=1, device_id={"gz": gz + 1}, device_id_type=MESH)

    for k in range(1, shot_count):
        peer = lax.rem(shot + k, shot_count)
        pl.semaphore_signal(barrier, inc=1, device_id={"shot": peer}, device_id_type=MESH)

    rows = lax.broadcasted_iota(jnp.int32, (nx, ny), 0)
    lanes = lax.broadcasted_iota(jnp.int32, (nx, ny), 1)
    cells = rows * ny + lanes

    def fx(a):
        return jnp.where(rows == nx - 1, 0.0, pltpu.roll(a, nx - 1, 0)) - a

    def bx(a):
        return a - jnp.where(rows == 0, 0.0, pltpu.roll(a, 1, 0))

    def fy(a):
        return jnp.where(lanes == ny - 1, 0.0, pltpu.roll(a, ny - 1, 1)) - a

    def by(a):
        return a - jnp.where(lanes == 0, 0.0, pltpu.roll(a, 1, 1))

    low_peers = (gz + gz_count - 1) // gz_count
    high_peers = (2 * gz_count - 2 - gz) // gz_count
    pl.semaphore_wait(barrier, low_peers + high_peers + shot_count - 1)

    def remote(src, dst, send, recv, step_to):
        return pltpu.make_async_remote_copy(
            src_ref=src,
            dst_ref=dst,
            send_sem=send,
            recv_sem=recv,
            device_id={"gz": gz + step_to},
            device_id_type=MESH,
        )

    def initial(src, dst, k, step_to):
        return remote(src, dst, init_send.at[k], init_recv.at[k], step_to)

    up_first = [initial(first_up.at[w], below.at[w], w, 1) for w in range(2)]
    up_earth = [initial(earth_up.at[i], below_earth.at[i], 2 + i, 1) for i in range(2)]
    down_first = [initial(first_szz.at[w], above.at[w, 4], 4 + w, -1) for w in range(2)]
    down_near = initial(earth_down.at[0], above_earth.at[0], 6, -1)
    down_far = [
        initial(earth_down, above_earth, 6, -1),
    ] + [
        initial(src, dst, 7 + 3 * w + i, -1)
        for w in range(2)
        for i, (src, dst) in enumerate(
            (
                (wave_hbm.at[0, w, pl.ds(VX, 2), 0], above.at[w, pl.ds(0, 2)]),
                (wave_hbm.at[0, w, pl.ds(SXX, 2), 0], above.at[w, pl.ds(2, 2)]),
                (wave_hbm.at[0, w, SXY, 0], above.at[w, 5]),
            )
        )
    ]

    for w in range(2):
        if w == 0:
            load_edge[0].wait()
        for copy in load_first[w]:
            copy.wait()
        szz, vz = state[w, SZZ, last], state[w, VZ, last]
        first_up[w, 2] = vz + (h * earth_up[0]) * (bx(first_up[w, 0]) + by(first_up[w, 1]) - szz)

        @pl.when(has_high)
        def _(w=w):
            up_first[w].start()
            if w == 0:
                up_earth[0].start()

        @pl.when(has_low)
        def _(w=w):
            down_first[w].start()

    for copy in load_edge[1:]:
        copy.wait()

    @pl.when(has_high)
    def _():
        up_earth[1].start()

    if paired:

        @pl.when(has_low & far)
        def _():
            for copy in down_far:
                copy.start()

        @pl.when(has_low & jnp.logical_not(far))
        def _():
            down_near.start()

    else:

        @pl.when(has_low)
        def _():
            down_near.start()

    @pl.when(jnp.logical_not(has_low))
    def _():
        below[...] = jnp.zeros_like(below)
        below_earth[...] = jnp.zeros_like(below_earth)
        low_in[...] = jnp.zeros_like(low_in)

    @pl.when(jnp.logical_not(has_high))
    def _():
        above[...] = jnp.zeros_like(above)
        above_earth[...] = jnp.zeros_like(above_earth)
        high_in[...] = jnp.zeros_like(high_in)
        rest_in[...] = jnp.zeros_like(rest_in)

    image[...] = jnp.zeros_like(image)
    load_earth.wait()
    earth[...] = earth[...] * h

    for copy in small:
        copy.wait()
    offset = gz * planes
    receivers = traces.shape[1]
    column = rec_column[...]
    depth = rec_depth[...] - offset
    row_ids = lax.broadcasted_iota(jnp.int32, (nx, receivers), 0) * ny
    past = column - row_ids
    on_row = (past >= 0) & (past < ny)
    row_hot = jnp.concatenate(
        [jnp.where(on_row & (depth == p), h, 0.0) for p in range(-1, planes)], axis=0
    )
    col_ids = lax.broadcasted_iota(jnp.int32, (ny, receivers), 0)
    col_hot = jnp.where((column & (ny - 1)) == col_ids, 1.0, 0.0)

    def fill(n, carry):
        inject[n] = lax.dot_general(
            row_hot * traces[pl.ds(n, 1), :],
            col_hot,
            (((1,), (1,)), ((), ())),
            precision=lax.Precision.HIGHEST,
            preferred_element_type=jnp.float32,
        ).reshape(planes + 1, nx, ny)
        return carry

    lax.fori_loop(0, steps, fill, 0)

    src_at = src_depth[0] - offset
    src_cell = src_column[0]

    def source_term(plane, n):
        cell = jnp.where(src_at == plane, src_cell, -1)
        return jnp.where(cells == cell, h * wavelet[0, n], 0.0)

    def parity(n):
        return n % 2 if isinstance(n, int) else lax.rem(n, 2)

    def send_up(w, n):
        return remote(up_out.at[w, n], low_in.at[w, n], up_send.at[w, n], up_recv.at[w, n], 1)

    def send_down(w, n):
        return remote(
            down_out.at[w, n], high_in.at[w, n], down_send.at[w, n], down_recv.at[w, n], -1
        )

    send_rest = remote(rest_out, rest_in, rest_sem.at[0], rest_sem.at[1], -1)

    def strains(w, p, n, vx, vy, dvz, hlam, hmu):
        ex, ey = bx(vx), by(vy)
        spread = hlam * (ex + ey + dvz)
        if w == 0:
            spread = spread + source_term(p, n)
        mu2 = 2.0 * hmu
        return spread + mu2 * ex, spread + mu2 * ey, spread + mu2 * dvz

    def a_node(w, p, n, final=False):
        hb, hlam, hmu = (earth[i, p] for i in range(3))
        sxy = state[w, SXY, p]
        below_p = (below[w, i] for i in range(3)) if p == 0 else (state[w, i, p - 1] for i in (SXZ, SYZ, VZ))
        sxz_b, syz_b, vz_b = below_p
        vx = state[w, VX, p] + hb * (fx(state[w, SXX, p]) + by(sxy) + (state[w, SXZ, p] - sxz_b))
        vy = state[w, VY, p] + hb * (bx(sxy) + fy(state[w, SYY, p]) + (state[w, SYZ, p] - syz_b))
        if w == 1 or not final:
            state[w, VX, p] = vx
            state[w, VY, p] = vy
        dxx, dyy, dzz = strains(w, p, n, vx, vy, state[w, VZ, p] - vz_b, hlam, hmu)
        sxx = state[w, SXX, p] + dxx
        syy = state[w, SYY, p] + dyy
        szz = state[w, SZZ, p] + dzz
        total = sxx + syy + szz
        if not final:
            state[w, SXX, p] = sxx
            state[w, SYY, p] = syy
            state[w, SZZ, p] = szz
        if w == 1 or not final:
            vxy, vyx = fy(vx), fx(vy)
        if not final:
            state[w, SXY, p] = sxy + hmu * (vxy + vyx)
        at = parity(n + 1)
        if w == 0:
            press[at, p] = total * (1.0 / (3 * steps))
        else:
            spin[p] = vyx - vxy
            image[pl.ds(p * nx, nx), :] += press[at, p] * (total * (1.0 / 3.0))
        return vx, vy, szz

    def curl(w, p, n, vxz, vyz, vzx, vzy):
        rotation = (vzy - vyz) + (vxz - vzx) + spin[p]
        image[pl.ds((planes + p) * nx, nx), :] += press[parity(n), p] * rotation

    def b_node(w, p, n, first, upper):
        hb, hmu = earth[0, p], earth[2, p]
        vz, sxz, syz = (state[w, i, p] for i in (VZ, SXZ, SYZ))
        vx_f, vy_f, szz_f = upper
        if not first:
            vxz, vyz = vx_f - state[w, VX, p], vy_f - state[w, VY, p]
            vzx, vzy = fx(vz), fy(vz)
            sxz = sxz + hmu * (vxz + vzx)
            syz = syz + hmu * (vyz + vzy)
            state[w, SXZ, p] = sxz
            state[w, SYZ, p] = syz
            if w == 1:
                curl(w, p, n, vxz, vyz, vzx, vzy)
        term = hb * (bx(sxz) + by(syz) + (szz_f - state[w, SZZ, p]))
        if w == 1:
            term = term + inject[n, p + 1]
        vz = vz + term
        state[w, VZ, p] = vz
        return sxz, syz, vz

    def own_upper(w, p):
        return tuple(state[w, i, p + 1] for i in (VX, VY, SZZ))

    def b_below(w, n, first):
        hb, hmu = below_earth[0], below_earth[1]
        vz = below[w, 2]
        if first:
            term = hb * state[w, SZZ, 0]
        else:
            vx_m, vy_m, szz_m = (low_in[w, n - 1, i] for i in range(3))
            sxz = below[w, 0] + hmu * ((state[w, VX, 0] - vx_m) + fx(vz))
            syz = below[w, 1] + hmu * ((state[w, VY, 0] - vy_m) + fy(vz))
            below[w, 0] = sxz
            below[w, 1] = syz
            term = hb * (bx(sxz) + by(syz) + (state[w, SZZ, 0] - szz_m))
        if w == 1:
            term = term + inject[n, 0]
        below[w, 2] = vz + term

    def above_velocity(w, sxz, syz):
        hb = above_earth[0]
        sxx, syy, sxy = above[w, 2], above[w, 3], above[w, 5]
        vx = above[w, 0] + hb * (fx(sxx) + by(sxy) + (sxz - state[w, SXZ, last]))
        vy = above[w, 1] + hb * (bx(sxy) + fy(syy) + (syz - state[w, SYZ, last]))
        return vx, vy

    def a_above(w, n):
        sxz, syz, vz = (high_in[w, n - 1, i] for i in range(3))
        hlam, hmu = above_earth[1], above_earth[2]
        vx, vy = above_velocity(w, sxz, syz)
        above[w, 0] = vx
        above[w, 1] = vy
        dxx, dyy, dzz = strains(w, planes, n - 1, vx, vy, vz - state[w, VZ, last], hlam, hmu)
        szz = above[w, 4] + dzz
        above[w, 2] += dxx
        above[w, 3] += dyy
        above[w, 4] = szz
        above[w, 5] += hmu * (fy(vx) + fx(vy))
        return vx, vy, szz

    inner = range(1, last)

    def run(deep):
        def inside(w, n):
            for p in range(1 if deep else 0, last):
                b_node(w, p, n, isinstance(n, int) and n == 0, own_upper(w, p))
            for p in inner:
                a_node(w, p, n)

        def store(buf, values, w, n):
            for i, value in enumerate(values):
                buf[w, n, i] = value

        def lowest_down(w, n):
            values = b_node(w, 0, n, isinstance(n, int) and n == 0, own_upper(w, 0))
            store(down_out, values, w, n)
            wanted = has_low if w == 1 else has_low & (n < steps - 1)

            @pl.when(wanted)
            def _():
                send_down(w, n).start()

        def half(w, n, first, final):
            if first:

                @pl.when(has_high)
                def _():
                    down_first[w].wait_recv()

            else:

                @pl.when(has_high)
                def _():
                    send_down(w, n - 1).wait_recv()

            def wait_low():
                @pl.when(has_low)
                def _():
                    if first:
                        up_first[w].wait_recv()
                        if w == 0:
                            up_earth[0].wait_recv()
                    else:
                        send_up(w, n - 1).wait_recv()

                if first and w == 0:
                    below_earth[0] = below_earth[0] * h

            if not deep:
                wait_low()
            if first:
                upper = (None, None, above[w, 4])
            elif deep:
                upper = a_above(w, n)
            else:
                upper = tuple(high_in[w, n - 1, i] for i in range(3))
            if deep:
                b_node(w, last, n, first, upper)
                values = a_node(w, last, n, final)
                if not final:
                    store(up_out, values, w, n)

                    @pl.when(has_high)
                    def _():
                        send_up(w, n).start()

                wait_low()
                b_below(w, n, first)
                a_node(w, 0, n, final)
                if not final:
                    lowest_down(w, n + 1)
            else:
                b_below(w, n, first)
                b_node(w, last, n, first, upper)
                lower = a_node(w, 0, n, final)
                values = a_node(w, last, n, final)
                if not final:
                    store(down_out, lower, w, n)
                    store(up_out, values, w, n)

                    @pl.when(has_low)
                    def _():
                        send_down(w, n).start()

                    @pl.when(has_high)
                    def _():
                        send_up(w, n).start()

            if not final:
                inside(w, n + 1)
                if w == 1 and not deep:

                    @pl.when(has_low & (n == steps - 2))
                    def _():
                        hb, sxy = earth[0, 0], state[1, SXY, 0]
                        rest_out[0] = state[1, VX, 0] + hb * (
                            fx(state[1, SXX, 0]) + by(sxy) + state[1, SXZ, 0]
                        )
                        rest_out[1] = state[1, VY, 0] + hb * (
                            bx(sxy) + fy(state[1, SYY, 0]) + state[1, SYZ, 0]
                        )
                        send_rest.start()

            elif w == 1:

                @pl.when(has_high)
                def _():
                    if deep:
                        send_down(1, n).wait_recv()
                    else:
                        send_rest.wait_recv()

                if deep:
                    vx_p, vy_p = above_velocity(1, high_in[1, n, 0], high_in[1, n, 1])
                else:
                    hb = above_earth[0]
                    vx_p = rest_in[0] - hb * state[1, SXZ, last]
                    vy_p = rest_in[1] - hb * state[1, SYZ, last]
                for p in range(planes):
                    vx_f = vx_p if p == last else state[1, VX, p + 1]
                    vy_f = vy_p if p == last else state[1, VY, p + 1]
                    vz = state[1, VZ, p]
                    curl(1, p, n + 1, vx_f - state[1, VX, p], vy_f - state[1, VY, p], fx(vz), fy(vz))

        for w in range(2):
            if deep:
                lowest_down(w, 0)
            inside(w, 0)
        for w in range(2):
            half(w, 0, True, False)

        @pl.when(has_low)
        def _():
            up_earth[1].wait_recv()

        below_earth[1] = below_earth[1] * h

        @pl.when(has_high)
        def _():
            for copy in down_far if deep else [down_near]:
                copy.wait_recv()

        for i in range(3 if deep else 1):
            above_earth[i] = above_earth[i] * h

        def body(n, carry):
            for w in range(2):
                half(w, n, False, False)
            return carry

        lax.fori_loop(1, steps - 1, body, 0)
        for w in range(2):
            half(w, steps - 1, False, True)

    if paired:
        pl.when(far)(lambda: run(True))
        pl.when(jnp.logical_not(far))(lambda: run(False))
    else:
        run(False)

    total = image.shape[0]
    chunk = total // shot_count

    def span(index):
        return pl.ds(pl.multiple_of(index * chunk, 8), chunk)

    scatter = []
    for k in range(1, shot_count):
        peer = lax.rem(shot + k, shot_count)
        copy = pltpu.make_async_remote_copy(
            src_ref=image.at[span(peer)],
            dst_ref=parts_in.at[k - 1],
            send_sem=img_send.at[0, k - 1],
            recv_sem=img_recv.at[0, k - 1],
            device_id={"shot": peer},
            device_id_type=MESH,
        )
        copy.start()
        scatter.append(copy)
    acc = image[span(shot), :]
    for k in range(1, shot_count):
        scatter[k - 1].wait_recv()
        acc = acc + parts_in[k - 1]
    own[...] = acc
    gather = []
    for k in range(1, shot_count):
        peer = lax.rem(shot + k, shot_count)
        copy = pltpu.make_async_remote_copy(
            src_ref=own,
            dst_ref=out.at[span(shot)],
            send_sem=img_send.at[1, k - 1],
            recv_sem=img_recv.at[1, k - 1],
            device_id={"shot": peer},
            device_id_type=MESH,
        )
        copy.start()
        gather.append(copy)
    out[span(shot), :] = acc

    @pl.when(has_high)
    def _():
        for copy in up_first + up_earth:
            copy.wait_send()

    @pl.when(has_low)
    def _():
        for copy in down_first:
            copy.wait_send()

    def drain_near():
        @pl.when(has_low)
        def _():
            down_near.wait_send()
            send_rest.wait_send()

    def drain_far():
        @pl.when(has_low)
        def _():
            for copy in down_far:
                copy.wait_send()
            send_down(1, steps - 1).wait_send()

    if paired:
        pl.when(far)(drain_far)
        pl.when(jnp.logical_not(far))(drain_near)
    else:
        drain_near()

    def drain(n, carry):
        for w in range(2):

            @pl.when(has_high)
            def _(w=w):
                send_up(w, n).wait_send()

            @pl.when(has_low)
            def _(w=w):
                send_down(w, n).wait_send()

        return carry

    lax.fori_loop(0, steps - 1, drain, 0)
    for copy in scatter:
        copy.wait_send()
    for copy in gather:
        copy.wait()


def on_device(
    gz_count,
    shot_count,
    wavefields,
    earth_model,
    source_depth,
    source_column,
    wavelet,
    receiver_depth,
    receiver_column,
    traces,
):
    planes, nx, ny = wavefields.shape[3:]
    steps = wavelet.shape[1]
    rows = 2 * planes * nx
    peers = max(shot_count - 1, 1)
    f32 = jnp.float32
    vmem = pl.BlockSpec(memory_space=pltpu.VMEM)
    hbm = pl.BlockSpec(memory_space=pltpu.HBM)
    dma = pltpu.SemaphoreType.DMA

    def plane(*lead):
        return pltpu.VMEM((*lead, nx, ny), f32)

    summed = pl.pallas_call(
        functools.partial(kernel, gz_count, shot_count),
        out_shape=jax.ShapeDtypeStruct((rows, ny), f32),
        in_specs=[hbm] * 8,
        out_specs=vmem,
        scratch_shapes=[
            plane(2, 9, planes),
            plane(3, planes),
            plane(2, 3),
            plane(2),
            plane(2, 6),
            plane(3),
            plane(2, 3),
            plane(2),
            plane(2),
            plane(3),
            plane(2, steps, 3),
            plane(2, steps, 3),
            plane(2, steps, 3),
            plane(2, steps, 3),
            plane(2),
            plane(2),
            plane(steps, planes + 1),
            plane(2, planes),
            plane(planes),
            pltpu.VMEM((rows, ny), f32),
            pltpu.VMEM((peers, rows // shot_count, ny), f32),
            pltpu.VMEM((rows // shot_count, ny), f32),
            pltpu.SMEM(source_depth.shape, jnp.int32),
            pltpu.SMEM(source_column.shape, jnp.int32),
            pltpu.SMEM(wavelet.shape, f32),
            pltpu.VMEM(receiver_depth.shape, jnp.int32),
            pltpu.VMEM(receiver_column.shape, jnp.int32),
            pltpu.VMEM(traces.shape[1:], f32),
            dma((18,)),
            dma((13,)),
            dma((13,)),
            dma((2, steps)),
            dma((2, steps)),
            dma((2, steps)),
            dma((2, steps)),
            dma((2,)),
            dma((2, peers)),
            dma((2, peers)),
        ],
        compiler_params=pltpu.CompilerParams(collective_id=0, has_side_effects=True),
    )(
        wavefields,
        earth_model,
        source_depth,
        source_column,
        wavelet,
        receiver_depth,
        receiver_column,
        traces,
    )
    return summed.reshape(2, planes, nx, ny)


def solution(mesh):
    placed = (
        P(("parts", "shot"), None, None, "gz", None, None),
        P("parts", "gz", None, None),
        P(("parts", "shot")),
        P(("parts", "shot")),
        P(("parts", "shot"), None),
        P(("parts", "shot"), None),
        P(("parts", "shot"), None),
        P(("parts", "shot"), None, None),
    )
    return jax.shard_map(
        functools.partial(on_device, mesh.shape["gz"], mesh.shape["shot"]),
        mesh=mesh,
        in_specs=placed,
        out_specs=P("parts", "gz", None, None),
        check_vma=False,
    )
```

```python
import functools

import jax
import jax.numpy as jnp
from jax import lax
from jax.experimental import pallas as pl
from jax.experimental.pallas import tpu as pltpu
from jax.sharding import PartitionSpec as P

time_step = 0.15
VX, VY, VZ, SXX, SYY, SZZ, SXY, SXZ, SYZ = range(9)
MESH = pl.DeviceIdType.MESH


def kernel(
    gz_count,
    shot_count,
    wave_hbm,
    earth_hbm,
    src_depth_hbm,
    src_column_hbm,
    wavelet_hbm,
    rec_depth_hbm,
    rec_column_hbm,
    traces_hbm,
    out,
    state,
    earth,
    below,
    below_earth,
    above,
    above_earth,
    first_up,
    first_szz,
    earth_up,
    earth_down,
    low_in,
    high_in,
    up_out,
    down_out,
    rest_in,
    rest_out,
    inject,
    press,
    spin,
    slope,
    grad,
    strain,
    twist,
    image,
    parts_in,
    own,
    src_depth,
    src_column,
    wavelet,
    rec_depth,
    rec_column,
    traces,
    load_sem,
    init_send,
    init_recv,
    up_send,
    up_recv,
    down_send,
    down_recv,
    rest_sem,
    img_send,
    img_recv,
):
    planes, nx, ny = state.shape[2:]
    steps = traces.shape[0]
    last = planes - 1
    h = time_step
    gz = lax.axis_index("gz")
    shot = lax.axis_index("shot")
    has_low = gz > 0
    has_high = gz < gz_count - 1
    paired = shot_count % 2 == 0
    far = lax.rem(shot, 2) == 0

    def local(src, dst, k):
        return pltpu.make_async_copy(src, dst, load_sem.at[k])

    load_first = [
        [
            local(wave_hbm.at[0, w, pl.ds(SXZ, 2), last], first_up.at[w, pl.ds(0, 2)], 4 * w),
            local(wave_hbm.at[0, w, SZZ, 0], first_szz.at[w], 4 * w + 1),
            local(wave_hbm.at[0, w], state.at[w], 4 * w + 2),
        ]
        for w in range(2)
    ]
    load_edge = [
        local(earth_hbm.at[0, last], earth_up.at[0], 8),
        local(earth_hbm.at[2, last], earth_up.at[1], 9),
        local(earth_hbm.at[:, 0], earth_down, 10),
    ]
    load_earth = local(earth_hbm, earth, 11)
    small = [
        local(src, dst, 12 + i)
        for i, (src, dst) in enumerate(
            (
                (traces_hbm.at[0], traces),
                (rec_depth_hbm, rec_depth),
                (rec_column_hbm, rec_column),
                (src_depth_hbm, src_depth),
                (src_column_hbm, src_column),
                (wavelet_hbm, wavelet),
            )
        )
    ]
    for copy in load_edge[:1] + load_first[0] + load_first[1] + load_edge[1:] + [load_earth] + small:
        copy.start()

    barrier = pltpu.get_barrier_semaphore()

    @pl.when(has_low)
    def _():
        pl.semaphore_signal(barrier, inc=1, device_id={"gz": gz - 1}, device_id_type=MESH)

    @pl.when(has_high)
    def _():
        pl.semaphore_signal(barrier, inc=1, device_id={"gz": gz + 1}, device_id_type=MESH)

    for k in range(1, shot_count):
        peer = lax.rem(shot + k, shot_count)
        pl.semaphore_signal(barrier, inc=1, device_id={"shot": peer}, device_id_type=MESH)

    rows = lax.broadcasted_iota(jnp.int32, (nx, ny), 0)
    lanes = lax.broadcasted_iota(jnp.int32, (nx, ny), 1)
    cells = rows * ny + lanes

    def fx(a):
        return jnp.where(rows == nx - 1, 0.0, pltpu.roll(a, nx - 1, 0)) - a

    def bx(a):
        return a - jnp.where(rows == 0, 0.0, pltpu.roll(a, 1, 0))

    def fy(a):
        return jnp.where(lanes == ny - 1, 0.0, pltpu.roll(a, ny - 1, 1)) - a

    def by(a):
        return a - jnp.where(lanes == 0, 0.0, pltpu.roll(a, 1, 1))

    low_peers = (gz + gz_count - 1) // gz_count
    high_peers = (2 * gz_count - 2 - gz) // gz_count
    pl.semaphore_wait(barrier, low_peers + high_peers + shot_count - 1)

    def remote(src, dst, send, recv, step_to):
        return pltpu.make_async_remote_copy(
            src_ref=src,
            dst_ref=dst,
            send_sem=send,
            recv_sem=recv,
            device_id={"gz": gz + step_to},
            device_id_type=MESH,
        )

    def initial(src, dst, k, step_to):
        return remote(src, dst, init_send.at[k], init_recv.at[k], step_to)

    up_first = [initial(first_up.at[w], below.at[w], w, 1) for w in range(2)]
    up_earth = [initial(earth_up.at[i], below_earth.at[i], 2 + i, 1) for i in range(2)]
    down_first = [initial(first_szz.at[w], above.at[w, 4], 4 + w, -1) for w in range(2)]
    down_near = initial(earth_down.at[0], above_earth.at[0], 6, -1)
    down_far = [
        initial(earth_down, above_earth, 6, -1),
    ] + [
        initial(src, dst, 7 + 3 * w + i, -1)
        for w in range(2)
        for i, (src, dst) in enumerate(
            (
                (wave_hbm.at[0, w, pl.ds(VX, 2), 0], above.at[w, pl.ds(0, 2)]),
                (wave_hbm.at[0, w, pl.ds(SXX, 2), 0], above.at[w, pl.ds(2, 2)]),
                (wave_hbm.at[0, w, SXY, 0], above.at[w, 5]),
            )
        )
    ]

    for w in range(2):
        if w == 0:
            load_edge[0].wait()
        for copy in load_first[w]:
            copy.wait()
        szz, vz = state[w, SZZ, last], state[w, VZ, last]
        first_up[w, 2] = vz + (h * earth_up[0]) * (bx(first_up[w, 0]) + by(first_up[w, 1]) - szz)

        @pl.when(has_high)
        def _(w=w):
            up_first[w].start()
            if w == 0:
                up_earth[0].start()

        @pl.when(has_low)
        def _(w=w):
            down_first[w].start()

    for copy in load_edge[1:]:
        copy.wait()

    @pl.when(has_high)
    def _():
        up_earth[1].start()

    if paired:

        @pl.when(has_low & far)
        def _():
            for copy in down_far:
                copy.start()

        @pl.when(has_low & jnp.logical_not(far))
        def _():
            down_near.start()

    else:

        @pl.when(has_low)
        def _():
            down_near.start()

    @pl.when(jnp.logical_not(has_low))
    def _():
        below[...] = jnp.zeros_like(below)
        below_earth[...] = jnp.zeros_like(below_earth)
        low_in[...] = jnp.zeros_like(low_in)

    @pl.when(jnp.logical_not(has_high))
    def _():
        above[...] = jnp.zeros_like(above)
        above_earth[...] = jnp.zeros_like(above_earth)
        high_in[...] = jnp.zeros_like(high_in)
        rest_in[...] = jnp.zeros_like(rest_in)

    image[...] = jnp.zeros_like(image)
    load_earth.wait()
    earth[...] = earth[...] * h

    for copy in small:
        copy.wait()
    offset = gz * planes
    receivers = traces.shape[1]
    column = rec_column[...]
    depth = rec_depth[...] - offset
    row_ids = lax.broadcasted_iota(jnp.int32, (nx, receivers), 0) * ny
    past = column - row_ids
    on_row = (past >= 0) & (past < ny)
    row_hot = jnp.concatenate(
        [jnp.where(on_row & (depth == p), h, 0.0) for p in range(-1, planes)], axis=0
    )
    col_ids = lax.broadcasted_iota(jnp.int32, (ny, receivers), 0)
    col_hot = jnp.where((column & (ny - 1)) == col_ids, 1.0, 0.0)

    def fill(n, carry):
        inject[n] = lax.dot_general(
            row_hot * traces[pl.ds(n, 1), :],
            col_hot,
            (((1,), (1,)), ((), ())),
            precision=lax.Precision.HIGHEST,
            preferred_element_type=jnp.float32,
        ).reshape(planes + 1, nx, ny)
        return carry

    lax.fori_loop(0, steps, fill, 0)

    src_at = src_depth[0] - offset
    src_cell = src_column[0]

    def source_term(plane, n):
        cell = jnp.where(src_at == plane, src_cell, -1)
        return jnp.where(cells == cell, h * wavelet[0, n], 0.0)

    def parity(n):
        return n % 2 if isinstance(n, int) else lax.rem(n, 2)

    def send_up(w, n):
        return remote(up_out.at[w, n], low_in.at[w, n], up_send.at[w, n], up_recv.at[w, n], 1)

    def send_down(w, n):
        return remote(
            down_out.at[w, n], high_in.at[w, n], down_send.at[w, n], down_recv.at[w, n], -1
        )

    send_rest = remote(rest_out, rest_in, rest_sem.at[0], rest_sem.at[1], -1)

    def strains(w, p, n, vx, vy, dvz, hlam, hmu):
        ex, ey = bx(vx), by(vy)
        spread = hlam * (ex + ey + dvz)
        if w == 0:
            spread = spread + source_term(p, n)
        mu2 = 2.0 * hmu
        return spread + mu2 * ex, spread + mu2 * ey, spread + mu2 * dvz

    def keep_pressure(w, p, n, total):
        at = parity(n + 1)
        if w == 0:
            press[at, p] = total * (1.0 / (3 * steps))
        else:
            image[pl.ds(p * nx, nx), :] += press[at, p] * (total * (1.0 / 3.0))

    def a_node(w, p, n):
        hb, hlam, hmu = (earth[i, p] for i in range(3))
        sxy = state[w, SXY, p]
        below_p = (below[w, i] for i in range(3)) if p == 0 else (state[w, i, p - 1] for i in (SXZ, SYZ, VZ))
        sxz_b, syz_b, vz_b = below_p
        vx = state[w, VX, p] + hb * (fx(state[w, SXX, p]) + by(sxy) + (state[w, SXZ, p] - sxz_b))
        vy = state[w, VY, p] + hb * (bx(sxy) + fy(state[w, SYY, p]) + (state[w, SYZ, p] - syz_b))
        state[w, VX, p] = vx
        state[w, VY, p] = vy
        dxx, dyy, dzz = strains(w, p, n, vx, vy, state[w, VZ, p] - vz_b, hlam, hmu)
        sxx = state[w, SXX, p] + dxx
        syy = state[w, SYY, p] + dyy
        szz = state[w, SZZ, p] + dzz
        total = sxx + syy + szz
        state[w, SXX, p] = sxx
        state[w, SYY, p] = syy
        state[w, SZZ, p] = szz
        vxy, vyx = fy(vx), fx(vy)
        state[w, SXY, p] = sxy + hmu * (vxy + vyx)
        keep_pressure(w, p, n, total)
        if w == 1:
            spin[p] = vyx - vxy

    def curl(w, p, n, vxz, vyz, vzx, vzy):
        rotation = (vzy - vyz) + (vxz - vzx) + spin[p]
        image[pl.ds((planes + p) * nx, nx), :] += press[parity(n), p] * rotation

    def b_node(w, p, n, first, upper):
        hb, hmu = earth[0, p], earth[2, p]
        vz, sxz, syz = (state[w, i, p] for i in (VZ, SXZ, SYZ))
        vx_f, vy_f, szz_f = upper
        if not first:
            vxz, vyz = vx_f - state[w, VX, p], vy_f - state[w, VY, p]
            vzx, vzy = fx(vz), fy(vz)
            sxz = sxz + hmu * (vxz + vzx)
            syz = syz + hmu * (vyz + vzy)
            state[w, SXZ, p] = sxz
            state[w, SYZ, p] = syz
            if w == 1:
                curl(w, p, n, vxz, vyz, vzx, vzy)
        term = hb * (bx(sxz) + by(syz) + (szz_f - state[w, SZZ, p]))
        if w == 1:
            term = term + inject[n, p + 1]
        vz = vz + term
        state[w, VZ, p] = vz
        return sxz, syz, vz

    def own_upper(w, p):
        return tuple(state[w, i, p + 1] for i in (VX, VY, SZZ))

    BELOW, LAST, LOWEST = range(3)
    ABOVE = 2

    def edge_at(p):
        return 0 if p == 0 else 1

    def set_slope(w, slot, vz):
        slope[w, slot, 0] = fx(vz)
        slope[w, slot, 1] = fy(vz)

    def set_grad(w, slot, sxx, syy, sxy):
        grad[w, slot, 0] = fx(sxx) + by(sxy)
        grad[w, slot, 1] = bx(sxy) + fy(syy)

    def edge_velocity(w, p):
        hb = earth[0, p]
        if p == 0:
            sxz_b, syz_b = below[w, 0], below[w, 1]
        else:
            sxz_b, syz_b = state[w, SXZ, p - 1], state[w, SYZ, p - 1]
        at = edge_at(p)
        vx = state[w, VX, p] + hb * (grad[w, at, 0] + (state[w, SXZ, p] - sxz_b))
        vy = state[w, VY, p] + hb * (grad[w, at, 1] + (state[w, SYZ, p] - syz_b))
        dvz = state[w, VZ, p] - (below[w, 2] if p == 0 else state[w, VZ, p - 1])
        return vx, vy, dvz

    def widen(w, at, p, n, vx, vy, dvz, hlam, hmu, szz):
        ey = by(vy)
        spread = hlam * (bx(vx) + ey + dvz)
        if w == 0:
            spread = spread + source_term(p, n)
        strain[w, at, 0] = spread
        strain[w, at, 1] = ey
        return szz + (spread + (2.0 * hmu) * dvz)

    def a_fast(w, p, n):
        vx, vy, dvz = edge_velocity(w, p)
        state[w, VX, p] = vx
        state[w, VY, p] = vy
        szz = widen(w, edge_at(p), p, n, vx, vy, dvz, earth[1, p], earth[2, p], state[w, SZZ, p])
        state[w, SZZ, p] = szz
        return vx, vy, szz

    def rest_of(w, at, vx, vy, hmu, sxx, syy, sxy):
        spread, mu2 = strain[w, at, 0], 2.0 * hmu
        vxy, vyx = fy(vx), fx(vy)
        sxx = sxx + (spread + mu2 * bx(vx))
        syy = syy + (spread + mu2 * strain[w, at, 1])
        sxy = sxy + hmu * (vxy + vyx)
        set_grad(w, at, sxx, syy, sxy)
        return sxx, syy, sxy, vyx - vxy

    def a_slow(w, p, n):
        sxx, syy, sxy, turn = rest_of(
            w, edge_at(p), *(state[w, i, p] for i in (VX, VY)), earth[2, p],
            *(state[w, i, p] for i in (SXX, SYY, SXY)),
        )
        state[w, SXX, p] = sxx
        state[w, SYY, p] = syy
        state[w, SXY, p] = sxy
        keep_pressure(w, p, n, sxx + syy + state[w, SZZ, p])
        if w == 1:
            spin[p] = turn

    def a_final(w, p, n):
        vx, vy, dvz = edge_velocity(w, p)
        volume = bx(vx) + by(vy) + dvz
        spread = earth[1, p] * volume
        if w == 0:
            spread = spread + source_term(p, n)
        total = state[w, SXX, p] + state[w, SYY, p] + state[w, SZZ, p]
        keep_pressure(w, p, n, total + (3.0 * spread + (2.0 * earth[2, p]) * volume))
        if w == 1:
            state[1, VX, p] = vx
            state[1, VY, p] = vy
            spin[p] = fx(vy) - fy(vx)

    def b_fast(w, p, slot, n, first, upper):
        hb, hmu = earth[0, p], earth[2, p]
        vz, sxz, syz = (state[w, i, p] for i in (VZ, SXZ, SYZ))
        vx_f, vy_f, szz_f = upper
        if not first:
            vxz, vyz = vx_f - state[w, VX, p], vy_f - state[w, VY, p]
            vzx, vzy = slope[w, slot, 0], slope[w, slot, 1]
            sxz = sxz + hmu * (vxz + vzx)
            syz = syz + hmu * (vyz + vzy)
            state[w, SXZ, p] = sxz
            state[w, SYZ, p] = syz
            if w == 1:
                twist[edge_at(p)] = (vzy - vyz) + (vxz - vzx)
        term = hb * (bx(sxz) + by(syz) + (szz_f - state[w, SZZ, p]))
        if w == 1:
            term = term + inject[n, p + 1]
        vz = vz + term
        state[w, VZ, p] = vz
        return sxz, syz, vz

    def keep_twist(p, n):
        image[pl.ds((planes + p) * nx, nx), :] += press[parity(n), p] * (
            twist[edge_at(p)] + spin[p]
        )

    def b_below(w, n, first):
        hb, hmu = below_earth[0], below_earth[1]
        vz = below[w, 2]
        if first:
            term = hb * state[w, SZZ, 0]
        else:
            vx_m, vy_m, szz_m = (low_in[w, n - 1, i] for i in range(3))
            sxz = below[w, 0] + hmu * ((state[w, VX, 0] - vx_m) + slope[w, BELOW, 0])
            syz = below[w, 1] + hmu * ((state[w, VY, 0] - vy_m) + slope[w, BELOW, 1])
            below[w, 0] = sxz
            below[w, 1] = syz
            term = hb * (bx(sxz) + by(syz) + (state[w, SZZ, 0] - szz_m))
        if w == 1:
            term = term + inject[n, 0]
        below[w, 2] = vz + term

    def above_velocity(w, sxz, syz):
        hb = above_earth[0]
        vx = above[w, 0] + hb * (grad[w, ABOVE, 0] + (sxz - state[w, SXZ, last]))
        vy = above[w, 1] + hb * (grad[w, ABOVE, 1] + (syz - state[w, SYZ, last]))
        return vx, vy

    def above_fast(w, n):
        sxz, syz, vz = (high_in[w, n - 1, i] for i in range(3))
        vx, vy = above_velocity(w, sxz, syz)
        above[w, 0] = vx
        above[w, 1] = vy
        dvz = vz - state[w, VZ, last]
        szz = widen(w, ABOVE, planes, n - 1, vx, vy, dvz, above_earth[1], above_earth[2], above[w, 4])
        above[w, 4] = szz
        return vx, vy, szz

    def above_slow(w):
        sxx, syy, sxy, _ = rest_of(
            w, ABOVE, above[w, 0], above[w, 1], above_earth[2], above[w, 2], above[w, 3], above[w, 5]
        )
        above[w, 2] = sxx
        above[w, 3] = syy
        above[w, 5] = sxy

    inner = range(1, last)

    def run(deep):
        def inside(w, n):
            for p in range(1 if deep else 0, last):
                b_node(w, p, n, isinstance(n, int) and n == 0, own_upper(w, p))
            for p in inner:
                a_node(w, p, n)

        def store(buf, values, w, n):
            for i, value in enumerate(values):
                buf[w, n, i] = value

        def lowest_down(w, n):
            values = b_fast(w, 0, LOWEST, n, isinstance(n, int) and n == 0, own_upper(w, 0))
            store(down_out, values, w, n)
            wanted = has_low if w == 1 else has_low & (n < steps - 1)

            @pl.when(wanted)
            def _():
                send_down(w, n).start()

        def half(w, n, first, final):
            if first:

                @pl.when(has_high)
                def _():
                    down_first[w].wait_recv()

            else:

                @pl.when(has_high)
                def _():
                    send_down(w, n - 1).wait_recv()

            def wait_low():
                @pl.when(has_low)
                def _():
                    if first:
                        up_first[w].wait_recv()
                        if w == 0:
                            up_earth[0].wait_recv()
                    else:
                        send_up(w, n - 1).wait_recv()

                if first and w == 0:
                    below_earth[0] = below_earth[0] * h

            if not deep:
                wait_low()
            if first:
                upper = (None, None, above[w, 4])
            elif deep:
                upper = above_fast(w, n)
            else:
                upper = tuple(high_in[w, n - 1, i] for i in range(3))
            if final:
                if deep:
                    wait_low()
                b_fast(w, last, LAST, n, first, upper)
                b_below(w, n, first)
                if w == 1:
                    keep_twist(last, n)
                    if deep:
                        above_slow(w)
                a_final(w, 0, n)
                a_final(w, last, n)
            elif deep:
                b_fast(w, last, LAST, n, first, upper)
                store(up_out, a_fast(w, last, n), w, n)

                @pl.when(has_high)
                def _():
                    send_up(w, n).start()

                wait_low()
                b_below(w, n, first)
                a_fast(w, 0, n)
                lowest_down(w, n + 1)
            else:
                b_below(w, n, first)
                b_fast(w, last, LAST, n, first, upper)
                store(down_out, a_fast(w, 0, n), w, n)
                store(up_out, a_fast(w, last, n), w, n)

                @pl.when(has_low)
                def _():
                    send_down(w, n).start()

                @pl.when(has_high)
                def _():
                    send_up(w, n).start()

            if not final:
                if w == 1 and not first:
                    keep_twist(last, n)
                a_slow(w, 0, n)
                a_slow(w, last, n)
                if deep:
                    if not first:
                        above_slow(w)
                    if w == 1:
                        keep_twist(0, n + 1)
                    set_slope(w, LOWEST, state[w, VZ, 0])
                set_slope(w, BELOW, below[w, 2])
                set_slope(w, LAST, state[w, VZ, last])
                inside(w, n + 1)
                if w == 1 and not deep:

                    @pl.when(has_low & (n == steps - 2))
                    def _():
                        hb = earth[0, 0]
                        rest_out[0] = state[1, VX, 0] + hb * (grad[1, 0, 0] + state[1, SXZ, 0])
                        rest_out[1] = state[1, VY, 0] + hb * (grad[1, 0, 1] + state[1, SYZ, 0])
                        send_rest.start()

            elif w == 1:

                @pl.when(has_high)
                def _():
                    if deep:
                        send_down(1, n).wait_recv()
                    else:
                        send_rest.wait_recv()

                if deep:
                    vx_p, vy_p = above_velocity(1, high_in[1, n, 0], high_in[1, n, 1])
                else:
                    hb = above_earth[0]
                    vx_p = rest_in[0] - hb * state[1, SXZ, last]
                    vy_p = rest_in[1] - hb * state[1, SYZ, last]
                for p in range(planes):
                    vx_f = vx_p if p == last else state[1, VX, p + 1]
                    vy_f = vy_p if p == last else state[1, VY, p + 1]
                    vz = state[1, VZ, p]
                    curl(1, p, n + 1, vx_f - state[1, VX, p], vy_f - state[1, VY, p], fx(vz), fy(vz))

        for w in range(2):
            if deep:
                lowest_down(w, 0)
                set_slope(w, LOWEST, state[w, VZ, 0])
            for p in sorted({0, last}):
                set_grad(w, edge_at(p), *(state[w, i, p] for i in (SXX, SYY, SXY)))
            inside(w, 0)
        for w in range(2):
            half(w, 0, True, False)

        @pl.when(has_low)
        def _():
            up_earth[1].wait_recv()

        below_earth[1] = below_earth[1] * h

        @pl.when(has_high)
        def _():
            for copy in down_far if deep else [down_near]:
                copy.wait_recv()

        for i in range(3 if deep else 1):
            above_earth[i] = above_earth[i] * h
        if deep:
            for w in range(2):
                set_grad(w, ABOVE, above[w, 2], above[w, 3], above[w, 5])

        def body(n, carry):
            for w in range(2):
                half(w, n, False, False)
            return carry

        lax.fori_loop(1, steps - 1, body, 0)
        for w in range(2):
            half(w, steps - 1, False, True)

    if paired:
        pl.when(far)(lambda: run(True))
        pl.when(jnp.logical_not(far))(lambda: run(False))
    else:
        run(False)

    total = image.shape[0]
    chunk = total // shot_count

    def span(index):
        return pl.ds(pl.multiple_of(index * chunk, 8), chunk)

    scatter = []
    for k in range(1, shot_count):
        peer = lax.rem(shot + k, shot_count)
        copy = pltpu.make_async_remote_copy(
            src_ref=image.at[span(peer)],
            dst_ref=parts_in.at[k - 1],
            send_sem=img_send.at[0, k - 1],
            recv_sem=img_recv.at[0, k - 1],
            device_id={"shot": peer},
            device_id_type=MESH,
        )
        copy.start()
        scatter.append(copy)
    acc = image[span(shot), :]
    for k in range(1, shot_count):
        scatter[k - 1].wait_recv()
        acc = acc + parts_in[k - 1]
    own[...] = acc
    gather = []
    for k in range(1, shot_count):
        peer = lax.rem(shot + k, shot_count)
        copy = pltpu.make_async_remote_copy(
            src_ref=own,
            dst_ref=out.at[span(shot)],
            send_sem=img_send.at[1, k - 1],
            recv_sem=img_recv.at[1, k - 1],
            device_id={"shot": peer},
            device_id_type=MESH,
        )
        copy.start()
        gather.append(copy)
    out[span(shot), :] = acc

    @pl.when(has_high)
    def _():
        for copy in up_first + up_earth:
            copy.wait_send()

    @pl.when(has_low)
    def _():
        for copy in down_first:
            copy.wait_send()

    def drain_near():
        @pl.when(has_low)
        def _():
            down_near.wait_send()
            send_rest.wait_send()

    def drain_far():
        @pl.when(has_low)
        def _():
            for copy in down_far:
                copy.wait_send()
            send_down(1, steps - 1).wait_send()

    if paired:
        pl.when(far)(drain_far)
        pl.when(jnp.logical_not(far))(drain_near)
    else:
        drain_near()

    def drain(n, carry):
        for w in range(2):

            @pl.when(has_high)
            def _(w=w):
                send_up(w, n).wait_send()

            @pl.when(has_low)
            def _(w=w):
                send_down(w, n).wait_send()

        return carry

    lax.fori_loop(0, steps - 1, drain, 0)
    for copy in scatter:
        copy.wait_send()
    for copy in gather:
        copy.wait()


def on_device(
    gz_count,
    shot_count,
    wavefields,
    earth_model,
    source_depth,
    source_column,
    wavelet,
    receiver_depth,
    receiver_column,
    traces,
):
    planes, nx, ny = wavefields.shape[3:]
    steps = wavelet.shape[1]
    rows = 2 * planes * nx
    peers = max(shot_count - 1, 1)
    f32 = jnp.float32
    vmem = pl.BlockSpec(memory_space=pltpu.VMEM)
    hbm = pl.BlockSpec(memory_space=pltpu.HBM)
    dma = pltpu.SemaphoreType.DMA

    def plane(*lead):
        return pltpu.VMEM((*lead, nx, ny), f32)

    summed = pl.pallas_call(
        functools.partial(kernel, gz_count, shot_count),
        out_shape=pltpu.VMEM((rows, ny), f32),
        in_specs=[hbm] * 8,
        out_specs=vmem,
        scratch_shapes=[
            plane(2, 9, planes),
            plane(3, planes),
            plane(2, 3),
            plane(2),
            plane(2, 6),
            plane(3),
            plane(2, 3),
            plane(2),
            plane(2),
            plane(3),
            plane(2, steps, 3),
            plane(2, steps, 3),
            plane(2, steps, 3),
            plane(2, steps, 3),
            plane(2),
            plane(2),
            plane(steps, planes + 1),
            plane(2, planes),
            plane(planes),
            plane(2, 3, 2),
            plane(2, 3, 2),
            plane(2, 3, 2),
            plane(2),
            pltpu.VMEM((rows, ny), f32),
            pltpu.VMEM((peers, rows // shot_count, ny), f32),
            pltpu.VMEM((rows // shot_count, ny), f32),
            pltpu.SMEM(source_depth.shape, jnp.int32),
            pltpu.SMEM(source_column.shape, jnp.int32),
            pltpu.SMEM(wavelet.shape, f32),
            pltpu.VMEM(receiver_depth.shape, jnp.int32),
            pltpu.VMEM(receiver_column.shape, jnp.int32),
            pltpu.VMEM(traces.shape[1:], f32),
            dma((18,)),
            dma((13,)),
            dma((13,)),
            dma((2, steps)),
            dma((2, steps)),
            dma((2, steps)),
            dma((2, steps)),
            dma((2,)),
            dma((2, peers)),
            dma((2, peers)),
        ],
        compiler_params=pltpu.CompilerParams(collective_id=0, has_side_effects=True),
    )(
        wavefields,
        earth_model,
        source_depth,
        source_column,
        wavelet,
        receiver_depth,
        receiver_column,
        traces,
    )
    return summed.reshape(2, planes, nx, ny)


def solution(mesh):
    placed = (
        P(("parts", "shot"), None, None, "gz", None, None),
        P("parts", "gz", None, None),
        P(("parts", "shot")),
        P(("parts", "shot")),
        P(("parts", "shot"), None),
        P(("parts", "shot"), None),
        P(("parts", "shot"), None),
        P(("parts", "shot"), None, None),
    )
    return jax.shard_map(
        functools.partial(on_device, mesh.shape["gz"], mesh.shape["shot"]),
        mesh=mesh,
        in_specs=placed,
        out_specs=P("parts", "gz", None, None),
        check_vma=False,
    )
```

```python
import functools

import jax
import jax.numpy as jnp
from jax import lax
from jax.experimental import pallas as pl
from jax.experimental.pallas import tpu as pltpu
from jax.sharding import PartitionSpec as P

time_step = 0.15
VX, VY, VZ, SXX, SYY, SZZ, SXY, SXZ, SYZ = range(9)
MESH = pl.DeviceIdType.MESH


def kernel(
    gz_count,
    shot_count,
    wave_hbm,
    earth_hbm,
    src_depth_hbm,
    src_column_hbm,
    wavelet_hbm,
    rec_depth_hbm,
    rec_column_hbm,
    traces_hbm,
    out,
    state,
    earth,
    below,
    below_earth,
    above,
    above_earth,
    first_up,
    first_szz,
    earth_up,
    earth_down,
    low_in,
    high_in,
    up_out,
    down_out,
    rest_in,
    rest_out,
    inject,
    press,
    spin,
    slope,
    grad,
    strain,
    twist,
    image,
    near_in,
    near_sum,
    cross_in,
    src_depth,
    src_column,
    wavelet,
    rec_depth,
    rec_column,
    traces,
    load_sem,
    init_send,
    init_recv,
    up_send,
    up_recv,
    down_send,
    down_recv,
    rest_sem,
    near_send,
    near_recv,
    cross_send,
    cross_recv,
):
    planes, nx, ny = state.shape[2:]
    steps = traces.shape[0]
    last = planes - 1
    h = time_step
    gz = lax.axis_index("gz")
    shot = lax.axis_index("shot")
    has_low = gz > 0
    has_high = gz < gz_count - 1
    paired = shot_count % 2 == 0
    far = lax.rem(shot, 2) == 0

    def local(src, dst, k):
        return pltpu.make_async_copy(src, dst, load_sem.at[k])

    load_first = [
        [
            local(wave_hbm.at[0, w, pl.ds(SXZ, 2), last], first_up.at[w, pl.ds(0, 2)], 4 * w),
            local(wave_hbm.at[0, w, SZZ, 0], first_szz.at[w], 4 * w + 1),
            local(wave_hbm.at[0, w], state.at[w], 4 * w + 2),
        ]
        for w in range(2)
    ]
    load_edge = [
        local(earth_hbm.at[0, last], earth_up.at[0], 8),
        local(earth_hbm.at[2, last], earth_up.at[1], 9),
        local(earth_hbm.at[:, 0], earth_down, 10),
    ]
    load_earth = local(earth_hbm, earth, 11)
    small = [
        local(src, dst, 12 + i)
        for i, (src, dst) in enumerate(
            (
                (traces_hbm.at[0], traces),
                (rec_depth_hbm, rec_depth),
                (rec_column_hbm, rec_column),
                (src_depth_hbm, src_depth),
                (src_column_hbm, src_column),
                (wavelet_hbm, wavelet),
            )
        )
    ]
    for copy in load_edge[:1] + load_first[0] + load_first[1] + load_edge[1:] + [load_earth] + small:
        copy.start()

    barrier = pltpu.get_barrier_semaphore()

    @pl.when(has_low)
    def _():
        pl.semaphore_signal(barrier, inc=1, device_id={"gz": gz - 1}, device_id_type=MESH)

    @pl.when(has_high)
    def _():
        pl.semaphore_signal(barrier, inc=1, device_id={"gz": gz + 1}, device_id_type=MESH)

    for k in range(1, shot_count):
        peer = lax.rem(shot + k, shot_count)
        pl.semaphore_signal(barrier, inc=1, device_id={"shot": peer}, device_id_type=MESH)

    rows = lax.broadcasted_iota(jnp.int32, (nx, ny), 0)
    lanes = lax.broadcasted_iota(jnp.int32, (nx, ny), 1)
    cells = rows * ny + lanes

    def fx(a):
        return jnp.where(rows == nx - 1, 0.0, pltpu.roll(a, nx - 1, 0)) - a

    def bx(a):
        return a - jnp.where(rows == 0, 0.0, pltpu.roll(a, 1, 0))

    def fy(a):
        return jnp.where(lanes == ny - 1, 0.0, pltpu.roll(a, ny - 1, 1)) - a

    def by(a):
        return a - jnp.where(lanes == 0, 0.0, pltpu.roll(a, 1, 1))

    low_peers = (gz + gz_count - 1) // gz_count
    high_peers = (2 * gz_count - 2 - gz) // gz_count
    pl.semaphore_wait(barrier, low_peers + high_peers + shot_count - 1)

    def remote(src, dst, send, recv, step_to):
        return pltpu.make_async_remote_copy(
            src_ref=src,
            dst_ref=dst,
            send_sem=send,
            recv_sem=recv,
            device_id={"gz": gz + step_to},
            device_id_type=MESH,
        )

    def initial(src, dst, k, step_to):
        return remote(src, dst, init_send.at[k], init_recv.at[k], step_to)

    up_first = [initial(first_up.at[w], below.at[w], w, 1) for w in range(2)]
    up_earth = [initial(earth_up.at[i], below_earth.at[i], 2 + i, 1) for i in range(2)]
    down_first = [initial(first_szz.at[w], above.at[w, 4], 4 + w, -1) for w in range(2)]
    down_near = initial(earth_down.at[0], above_earth.at[0], 6, -1)
    down_far = [
        initial(earth_down, above_earth, 6, -1),
    ] + [
        initial(src, dst, 7 + 3 * w + i, -1)
        for w in range(2)
        for i, (src, dst) in enumerate(
            (
                (wave_hbm.at[0, w, pl.ds(VX, 2), 0], above.at[w, pl.ds(0, 2)]),
                (wave_hbm.at[0, w, pl.ds(SXX, 2), 0], above.at[w, pl.ds(2, 2)]),
                (wave_hbm.at[0, w, SXY, 0], above.at[w, 5]),
            )
        )
    ]

    for w in range(2):
        if w == 0:
            load_edge[0].wait()
        for copy in load_first[w]:
            copy.wait()
        szz, vz = state[w, SZZ, last], state[w, VZ, last]
        first_up[w, 2] = vz + (h * earth_up[0]) * (bx(first_up[w, 0]) + by(first_up[w, 1]) - szz)

        @pl.when(has_high)
        def _(w=w):
            up_first[w].start()
            if w == 0:
                up_earth[0].start()

        @pl.when(has_low)
        def _(w=w):
            down_first[w].start()

    for copy in load_edge[1:]:
        copy.wait()

    @pl.when(has_high)
    def _():
        up_earth[1].start()

    if paired:

        @pl.when(has_low & far)
        def _():
            for copy in down_far:
                copy.start()

        @pl.when(has_low & jnp.logical_not(far))
        def _():
            down_near.start()

    else:

        @pl.when(has_low)
        def _():
            down_near.start()

    @pl.when(jnp.logical_not(has_low))
    def _():
        below[...] = jnp.zeros_like(below)
        below_earth[...] = jnp.zeros_like(below_earth)
        low_in[...] = jnp.zeros_like(low_in)

    @pl.when(jnp.logical_not(has_high))
    def _():
        above[...] = jnp.zeros_like(above)
        above_earth[...] = jnp.zeros_like(above_earth)
        high_in[...] = jnp.zeros_like(high_in)
        rest_in[...] = jnp.zeros_like(rest_in)

    image[...] = jnp.zeros_like(image)
    load_earth.wait()
    earth[...] = earth[...] * h

    for copy in small:
        copy.wait()
    offset = gz * planes
    receivers = traces.shape[1]
    column = rec_column[...]
    depth = rec_depth[...] - offset
    row_ids = lax.broadcasted_iota(jnp.int32, (nx, receivers), 0) * ny
    past = column - row_ids
    on_row = (past >= 0) & (past < ny)
    row_hot = jnp.concatenate(
        [jnp.where(on_row & (depth == p), h, 0.0) for p in range(-1, planes)], axis=0
    )
    col_ids = lax.broadcasted_iota(jnp.int32, (ny, receivers), 0)
    col_hot = jnp.where((column & (ny - 1)) == col_ids, 1.0, 0.0)

    def fill(n, carry):
        inject[n] = lax.dot_general(
            row_hot * traces[pl.ds(n, 1), :],
            col_hot,
            (((1,), (1,)), ((), ())),
            precision=lax.Precision.HIGHEST,
            preferred_element_type=jnp.float32,
        ).reshape(planes + 1, nx, ny)
        return carry

    lax.fori_loop(0, steps, fill, 0)

    src_at = src_depth[0] - offset
    src_cell = src_column[0]

    def source_term(plane, n):
        cell = jnp.where(src_at == plane, src_cell, -1)
        return jnp.where(cells == cell, h * wavelet[0, n], 0.0)

    def parity(n):
        return n % 2 if isinstance(n, int) else lax.rem(n, 2)

    def part_of(ref, w, n, part):
        return ref.at[w, n, pl.ds(0, 2)] if part == 0 else ref.at[w, n, 2]

    def send_up(w, n, part):
        return remote(
            part_of(up_out, w, n, part),
            part_of(low_in, w, n, part),
            up_send.at[w, n, part],
            up_recv.at[w, n, part],
            1,
        )

    def send_down(w, n, part):
        return remote(
            part_of(down_out, w, n, part),
            part_of(high_in, w, n, part),
            down_send.at[w, n, part],
            down_recv.at[w, n, part],
            -1,
        )

    send_rest = remote(rest_out, rest_in, rest_sem.at[0], rest_sem.at[1], -1)

    def strains(w, p, n, vx, vy, dvz, hlam, hmu):
        ex, ey = bx(vx), by(vy)
        spread = hlam * (ex + ey + dvz)
        if w == 0:
            spread = spread + source_term(p, n)
        mu2 = 2.0 * hmu
        return spread + mu2 * ex, spread + mu2 * ey, spread + mu2 * dvz

    def keep_pressure(w, p, n, total):
        at = parity(n + 1)
        if w == 0:
            press[at, p] = total * (1.0 / (3 * steps))
        else:
            image[pl.ds(p * nx, nx), :] += press[at, p] * (total * (1.0 / 3.0))

    def a_node(w, p, n):
        hb, hlam, hmu = (earth[i, p] for i in range(3))
        sxy = state[w, SXY, p]
        below_p = (below[w, i] for i in range(3)) if p == 0 else (state[w, i, p - 1] for i in (SXZ, SYZ, VZ))
        sxz_b, syz_b, vz_b = below_p
        vx = state[w, VX, p] + hb * (fx(state[w, SXX, p]) + by(sxy) + (state[w, SXZ, p] - sxz_b))
        vy = state[w, VY, p] + hb * (bx(sxy) + fy(state[w, SYY, p]) + (state[w, SYZ, p] - syz_b))
        state[w, VX, p] = vx
        state[w, VY, p] = vy
        dxx, dyy, dzz = strains(w, p, n, vx, vy, state[w, VZ, p] - vz_b, hlam, hmu)
        sxx = state[w, SXX, p] + dxx
        syy = state[w, SYY, p] + dyy
        szz = state[w, SZZ, p] + dzz
        total = sxx + syy + szz
        state[w, SXX, p] = sxx
        state[w, SYY, p] = syy
        state[w, SZZ, p] = szz
        vxy, vyx = fy(vx), fx(vy)
        state[w, SXY, p] = sxy + hmu * (vxy + vyx)
        keep_pressure(w, p, n, total)
        if w == 1:
            spin[p] = vyx - vxy

    def curl(w, p, n, vxz, vyz, vzx, vzy):
        rotation = (vzy - vyz) + (vxz - vzx) + spin[p]
        image[pl.ds((planes + p) * nx, nx), :] += press[parity(n), p] * rotation

    def b_node(w, p, n, first, upper):
        hb, hmu = earth[0, p], earth[2, p]
        vz, sxz, syz = (state[w, i, p] for i in (VZ, SXZ, SYZ))
        vx_f, vy_f, szz_f = upper
        if not first:
            vxz, vyz = vx_f - state[w, VX, p], vy_f - state[w, VY, p]
            vzx, vzy = fx(vz), fy(vz)
            sxz = sxz + hmu * (vxz + vzx)
            syz = syz + hmu * (vyz + vzy)
            state[w, SXZ, p] = sxz
            state[w, SYZ, p] = syz
            if w == 1:
                curl(w, p, n, vxz, vyz, vzx, vzy)
        term = hb * (bx(sxz) + by(syz) + (szz_f - state[w, SZZ, p]))
        if w == 1:
            term = term + inject[n, p + 1]
        vz = vz + term
        state[w, VZ, p] = vz
        return sxz, syz, vz

    def own_upper(w, p):
        return tuple(state[w, i, p + 1] for i in (VX, VY, SZZ))

    BELOW, LAST, LOWEST = range(3)
    ABOVE = 2

    def edge_at(p):
        return 0 if p == 0 else 1

    def set_slope(w, slot, vz):
        slope[w, slot, 0] = fx(vz)
        slope[w, slot, 1] = fy(vz)

    def set_grad(w, slot, sxx, syy, sxy):
        grad[w, slot, 0] = fx(sxx) + by(sxy)
        grad[w, slot, 1] = bx(sxy) + fy(syy)

    def edge_velocity(w, p):
        hb = earth[0, p]
        if p == 0:
            sxz_b, syz_b = below[w, 0], below[w, 1]
        else:
            sxz_b, syz_b = state[w, SXZ, p - 1], state[w, SYZ, p - 1]
        at = edge_at(p)
        vx = state[w, VX, p] + hb * (grad[w, at, 0] + (state[w, SXZ, p] - sxz_b))
        vy = state[w, VY, p] + hb * (grad[w, at, 1] + (state[w, SYZ, p] - syz_b))
        return vx, vy

    def edge_rise(w, p):
        return state[w, VZ, p] - (below[w, 2] if p == 0 else state[w, VZ, p - 1])

    def widen(w, at, p, n, vx, vy, hlam, hmu):
        ey = by(vy)
        strain[w, at, 1] = ey
        flat = bx(vx) + ey

        def finish(dvz):
            spread = hlam * (flat + dvz)
            if w == 0:
                spread = spread + source_term(p, n)
            strain[w, at, 0] = spread
            return spread + (2.0 * hmu) * dvz

        return finish

    def a_fast(w, p, n):
        vx, vy = edge_velocity(w, p)
        state[w, VX, p] = vx
        state[w, VY, p] = vy
        change = widen(w, edge_at(p), p, n, vx, vy, earth[1, p], earth[2, p])

        def finish():
            szz = state[w, SZZ, p] + change(edge_rise(w, p))
            state[w, SZZ, p] = szz
            return szz

        return (vx, vy), finish

    def rest_of(w, at, vx, vy, hmu, sxx, syy, sxy):
        spread, mu2 = strain[w, at, 0], 2.0 * hmu
        vxy, vyx = fy(vx), fx(vy)
        sxx = sxx + (spread + mu2 * bx(vx))
        syy = syy + (spread + mu2 * strain[w, at, 1])
        sxy = sxy + hmu * (vxy + vyx)
        set_grad(w, at, sxx, syy, sxy)
        return sxx, syy, sxy, vyx - vxy

    def a_slow(w, p, n):
        sxx, syy, sxy, turn = rest_of(
            w, edge_at(p), *(state[w, i, p] for i in (VX, VY)), earth[2, p],
            *(state[w, i, p] for i in (SXX, SYY, SXY)),
        )
        state[w, SXX, p] = sxx
        state[w, SYY, p] = syy
        state[w, SXY, p] = sxy
        keep_pressure(w, p, n, sxx + syy + state[w, SZZ, p])
        if w == 1:
            spin[p] = turn

    def a_final(w, p, n):
        vx, vy = edge_velocity(w, p)
        volume = bx(vx) + by(vy) + edge_rise(w, p)
        spread = earth[1, p] * volume
        if w == 0:
            spread = spread + source_term(p, n)
        total = state[w, SXX, p] + state[w, SYY, p] + state[w, SZZ, p]
        keep_pressure(w, p, n, total + (3.0 * spread + (2.0 * earth[2, p]) * volume))
        if w == 1:
            state[1, VX, p] = vx
            state[1, VY, p] = vy
            spin[p] = fx(vy) - fy(vx)

    def b_fast(w, p, slot, n, first, vx_f, vy_f):
        sxz, syz = state[w, SXZ, p], state[w, SYZ, p]
        if not first:
            hmu = earth[2, p]
            vxz, vyz = vx_f - state[w, VX, p], vy_f - state[w, VY, p]
            vzx, vzy = slope[w, slot, 0], slope[w, slot, 1]
            sxz = sxz + hmu * (vxz + vzx)
            syz = syz + hmu * (vyz + vzy)
            state[w, SXZ, p] = sxz
            state[w, SYZ, p] = syz
            if w == 1:
                twist[edge_at(p)] = (vzy - vyz) + (vxz - vzx)

        def flat():
            return bx(sxz) + by(syz)

        def finish(shear, szz_f):
            term = earth[0, p] * (shear + (szz_f - state[w, SZZ, p]))
            if w == 1:
                term = term + inject[n, p + 1]
            vz = state[w, VZ, p] + term
            state[w, VZ, p] = vz
            return vz

        return (sxz, syz), flat, finish

    def keep_twist(p, n):
        image[pl.ds((planes + p) * nx, nx), :] += press[parity(n), p] * (
            twist[edge_at(p)] + spin[p]
        )

    def b_below(w, n, first):
        if not first:
            hmu = below_earth[1]
            vx_m, vy_m = low_in[w, n - 1, 0], low_in[w, n - 1, 1]
            sxz = below[w, 0] + hmu * ((state[w, VX, 0] - vx_m) + slope[w, BELOW, 0])
            syz = below[w, 1] + hmu * ((state[w, VY, 0] - vy_m) + slope[w, BELOW, 1])
            below[w, 0] = sxz
            below[w, 1] = syz

        def flat():
            return None if first else bx(sxz) + by(syz)

        def finish(shear):
            szz = state[w, SZZ, 0]
            term = below_earth[0] * (szz if first else shear + (szz - low_in[w, n - 1, 2]))
            if w == 1:
                term = term + inject[n, 0]
            below[w, 2] = below[w, 2] + term

        return flat, finish

    def above_velocity(w, sxz, syz):
        hb = above_earth[0]
        vx = above[w, 0] + hb * (grad[w, ABOVE, 0] + (sxz - state[w, SXZ, last]))
        vy = above[w, 1] + hb * (grad[w, ABOVE, 1] + (syz - state[w, SYZ, last]))
        return vx, vy

    def above_fast(w, n):
        vx, vy = above_velocity(w, high_in[w, n - 1, 0], high_in[w, n - 1, 1])
        above[w, 0] = vx
        above[w, 1] = vy
        change = widen(w, ABOVE, planes, n - 1, vx, vy, above_earth[1], above_earth[2])

        def finish():
            szz = above[w, 4] + change(high_in[w, n - 1, 2] - state[w, VZ, last])
            above[w, 4] = szz
            return szz

        return (vx, vy), finish

    def above_slow(w):
        sxx, syy, sxy, _ = rest_of(
            w, ABOVE, above[w, 0], above[w, 1], above_earth[2], above[w, 2], above[w, 3], above[w, 5]
        )
        above[w, 2] = sxx
        above[w, 3] = syy
        above[w, 5] = sxy

    inner = range(1, last)
    bounds = [(nx, last * nx), ((planes + 1) * nx, (planes + last - 1) * nx)]
    early = [i for i in range(2) if bounds[i][1] > bounds[i][0]]
    bounds += [(0, nx), (last * nx, (planes + 1) * nx), ((planes + last - 1) * nx, 2 * planes * nx)]
    late = [2, 3, 4]
    pairs = shot_count // 2 if paired else shot_count

    def piece(i):
        return pl.ds(bounds[i][0], bounds[i][1] - bounds[i][0])

    def to_shot(src, dst, send, recv, target):
        return pltpu.make_async_remote_copy(
            src_ref=src,
            dst_ref=dst,
            send_sem=send,
            recv_sem=recv,
            device_id={"shot": target},
            device_id_type=MESH,
        )

    def gather_pair(i):
        sems = near_send.at[0, i], near_recv.at[0, i]
        return to_shot(image.at[piece(i)], near_in.at[piece(i)], *sems, shot + 1)

    def give_back(i):
        sems = near_send.at[1, i], near_recv.at[1, i]
        return to_shot(out.at[piece(i)], out.at[piece(i)], *sems, shot - 1)

    def cross(i, k):
        target = lax.rem(shot + k * (shot_count // pairs), shot_count)
        sems = cross_send.at[k - 1, i], cross_recv.at[k - 1, i]
        return to_shot(near_sum.at[piece(i)], cross_in.at[k - 1, piece(i)], *sems, target)

    def merge_pair(i):
        if paired:
            gather_pair(i).wait_recv()
            near_sum[piece(i), :] = image[piece(i), :] + near_in[piece(i), :]
        else:
            near_sum[piece(i), :] = image[piece(i), :]
        for k in range(1, pairs):
            cross(i, k).start()

    def merge_all(i):
        total = near_sum[piece(i), :]
        for k in range(1, pairs):
            cross(i, k).wait_recv()
            total = total + cross_in[k - 1, piece(i), :]
        out[piece(i), :] = total
        if paired:
            give_back(i).start()

    def run(deep):
        def inside(w, n):
            for p in range(1 if deep else 0, last):
                b_node(w, p, n, isinstance(n, int) and n == 0, own_upper(w, p))
            for p in inner:
                a_node(w, p, n)

        def store(buf, values, w, n):
            for i, value in enumerate(values):
                buf[w, n, i] = value

        def start_up(w, n, part):
            @pl.when(has_high)
            def _():
                send_up(w, n, part).start()

        def start_down(w, n, part):
            wanted = has_low
            if deep and (w == 0 or part == 1):
                wanted = has_low & (n < steps - 1)

            @pl.when(wanted)
            def _():
                send_down(w, n, part).start()

        def wait_high(w, n, part):
            @pl.when(has_high)
            def _():
                send_down(w, n, part).wait_recv()

        def wait_low(w, n, part):
            @pl.when(has_low)
            def _():
                send_up(w, n, part).wait_recv()

        def first_low(w):
            @pl.when(has_low)
            def _():
                up_first[w].wait_recv()
                if w == 0:
                    up_earth[0].wait_recv()

            if w == 0:
                below_earth[0] = below_earth[0] * h

        def half(w, n, first, final):
            if first:

                @pl.when(has_high)
                def _():
                    down_first[w].wait_recv()

                szz_f = above[w, 4]
            vx_f = vy_f = None
            if final:
                for part in range(2):
                    wait_high(w, n - 1, part)
                    wait_low(w, n - 1, part)
                if deep:
                    (vx_f, vy_f), lift = above_fast(w, n)
                    szz_f = lift()
                else:
                    vx_f, vy_f, szz_f = (high_in[w, n - 1, i] for i in range(3))
                _, shear, rise = b_fast(w, last, LAST, n, first, vx_f, vy_f)
                rise(shear(), szz_f)
                shear, rise = b_below(w, n, first)
                rise(shear())
                if w == 1:
                    keep_twist(last, n)
                    if deep:
                        above_slow(w)
                a_final(w, 0, n)
                a_final(w, last, n)
            elif deep:
                if not first:
                    wait_high(w, n - 1, 0)
                    (vx_f, vy_f), lift = above_fast(w, n)
                _, shear, rise = b_fast(w, last, LAST, n, first, vx_f, vy_f)
                values, top = a_fast(w, last, n)
                store(up_out, values, w, n)
                start_up(w, n, 0)
                shear = shear()
                if not first:
                    wait_high(w, n - 1, 1)
                    szz_f = lift()
                rise(shear, szz_f)
                up_out[w, n, 2] = top()
                start_up(w, n, 1)
                if first:
                    first_low(w)
                else:
                    wait_low(w, n - 1, 0)
                shear_m, rise_m = b_below(w, n, first)
                _, bottom = a_fast(w, 0, n)
                lower = (state[w, VX, 1], state[w, VY, 1])
                values, shear, rise = b_fast(w, 0, LOWEST, n + 1, False, *lower)
                store(down_out, values, w, n + 1)
                start_down(w, n + 1, 0)
                shear_m, shear = shear_m(), shear()
                if not first:
                    wait_low(w, n - 1, 1)
                rise_m(shear_m)
                bottom()
                down_out[w, n + 1, 2] = rise(shear, state[w, SZZ, 1])
                start_down(w, n + 1, 1)
            else:
                if first:
                    first_low(w)
                else:
                    wait_low(w, n - 1, 0)
                    wait_high(w, n - 1, 0)
                    vx_f, vy_f = high_in[w, n - 1, 0], high_in[w, n - 1, 1]
                shear_m, rise_m = b_below(w, n, first)
                _, shear, rise = b_fast(w, last, LAST, n, first, vx_f, vy_f)
                values, bottom = a_fast(w, 0, n)
                store(down_out, values, w, n)
                values, top = a_fast(w, last, n)
                store(up_out, values, w, n)
                start_down(w, n, 0)
                start_up(w, n, 0)
                shear_m, shear = shear_m(), shear()
                if not first:
                    wait_low(w, n - 1, 1)
                    wait_high(w, n - 1, 1)
                    szz_f = high_in[w, n - 1, 2]
                rise_m(shear_m)
                rise(shear, szz_f)
                down_out[w, n, 2] = bottom()
                up_out[w, n, 2] = top()
                start_down(w, n, 1)
                start_up(w, n, 1)

            if not final:
                if w == 1 and not first:
                    keep_twist(last, n)
                a_slow(w, 0, n)
                a_slow(w, last, n)
                if deep:
                    if not first:
                        above_slow(w)
                    if w == 1:
                        keep_twist(0, n + 1)
                    set_slope(w, LOWEST, state[w, VZ, 0])
                set_slope(w, BELOW, below[w, 2])
                set_slope(w, LAST, state[w, VZ, last])
                inside(w, n + 1)
                if w == 1 and not deep:

                    @pl.when(has_low & (n == steps - 2))
                    def _():
                        hb = earth[0, 0]
                        rest_out[0] = state[1, VX, 0] + hb * (grad[1, 0, 0] + state[1, SXZ, 0])
                        rest_out[1] = state[1, VY, 0] + hb * (grad[1, 0, 1] + state[1, SYZ, 0])
                        send_rest.start()

            elif w == 1:

                @pl.when(has_high)
                def _():
                    if deep:
                        send_down(1, n, 0).wait_recv()
                    else:
                        send_rest.wait_recv()

                if deep:
                    vx_p, vy_p = above_velocity(1, high_in[1, n, 0], high_in[1, n, 1])
                else:
                    hb = above_earth[0]
                    vx_p = rest_in[0] - hb * state[1, SXZ, last]
                    vy_p = rest_in[1] - hb * state[1, SYZ, last]
                for p in range(planes):
                    if 0 < p < last - 1:
                        continue
                    vx_f = vx_p if p == last else state[1, VX, p + 1]
                    vy_f = vy_p if p == last else state[1, VY, p + 1]
                    vz = state[1, VZ, p]
                    curl(1, p, n + 1, vx_f - state[1, VX, p], vy_f - state[1, VY, p], fx(vz), fy(vz))

        for w in range(2):
            if deep:
                values, shear, rise = b_fast(w, 0, LOWEST, 0, True, None, None)
                store(down_out, values, w, 0)
                start_down(w, 0, 0)
                down_out[w, 0, 2] = rise(shear(), state[w, SZZ, 1])
                start_down(w, 0, 1)
                set_slope(w, LOWEST, state[w, VZ, 0])
            for p in sorted({0, last}):
                set_grad(w, edge_at(p), *(state[w, i, p] for i in (SXX, SYY, SXY)))
            inside(w, 0)
        for w in range(2):
            half(w, 0, True, False)

        @pl.when(has_low)
        def _():
            up_earth[1].wait_recv()

        below_earth[1] = below_earth[1] * h

        @pl.when(has_high)
        def _():
            for copy in down_far if deep else [down_near]:
                copy.wait_recv()

        for i in range(3 if deep else 1):
            above_earth[i] = above_earth[i] * h
        if deep:
            for w in range(2):
                set_grad(w, ABOVE, above[w, 2], above[w, 3], above[w, 5])

        def body(n, carry):
            for w in range(2):
                half(w, n, False, False)
            return carry

        lax.fori_loop(1, steps - 1, body, 0)
        for p in range(1, last - 1):
            vx, vy, vz = (state[1, i, p] for i in (VX, VY, VZ))
            curl(1, p, steps, state[1, VX, p + 1] - vx, state[1, VY, p + 1] - vy, fx(vz), fy(vz))
        if deep:
            for i in early:
                gather_pair(i).start()
        half(0, steps - 1, False, True)
        if not deep:
            for i in early:
                merge_pair(i)
        half(1, steps - 1, False, True)
        if deep:
            for i in late:
                gather_pair(i).start()
            for i in early + late:
                give_back(i).wait_recv()
            for i in early + late:
                gather_pair(i).wait_send()
        else:
            for i in late:
                merge_pair(i)
            for i in early + late:
                merge_all(i)
            for i in early + late:
                for k in range(1, pairs):
                    cross(i, k).wait_send()
                if paired:
                    give_back(i).wait_send()

    if paired:
        pl.when(far)(lambda: run(True))
        pl.when(jnp.logical_not(far))(lambda: run(False))
    else:
        run(False)

    @pl.when(has_high)
    def _():
        for copy in up_first + up_earth:
            copy.wait_send()

    @pl.when(has_low)
    def _():
        for copy in down_first:
            copy.wait_send()

    def drain_near():
        @pl.when(has_low)
        def _():
            down_near.wait_send()
            send_rest.wait_send()

    def drain_far():
        @pl.when(has_low)
        def _():
            for copy in down_far:
                copy.wait_send()
            send_down(1, steps - 1, 0).wait_send()

    if paired:
        pl.when(far)(drain_far)
        pl.when(jnp.logical_not(far))(drain_near)
    else:
        drain_near()

    def drain(n, carry):
        for w in range(2):

            @pl.when(has_high)
            def _(w=w):
                for part in range(2):
                    send_up(w, n, part).wait_send()

            @pl.when(has_low)
            def _(w=w):
                for part in range(2):
                    send_down(w, n, part).wait_send()

        return carry

    lax.fori_loop(0, steps - 1, drain, 0)


def on_device(
    gz_count,
    shot_count,
    wavefields,
    earth_model,
    source_depth,
    source_column,
    wavelet,
    receiver_depth,
    receiver_column,
    traces,
):
    planes, nx, ny = wavefields.shape[3:]
    steps = wavelet.shape[1]
    rows = 2 * planes * nx
    groups = max((shot_count + 1) // 2 - 1, 1)
    f32 = jnp.float32
    vmem = pl.BlockSpec(memory_space=pltpu.VMEM)
    hbm = pl.BlockSpec(memory_space=pltpu.HBM)
    dma = pltpu.SemaphoreType.DMA

    def plane(*lead):
        return pltpu.VMEM((*lead, nx, ny), f32)

    summed = pl.pallas_call(
        functools.partial(kernel, gz_count, shot_count),
        out_shape=pltpu.VMEM((rows, ny), f32),
        in_specs=[hbm] * 8,
        out_specs=vmem,
        scratch_shapes=[
            plane(2, 9, planes),
            plane(3, planes),
            plane(2, 3),
            plane(2),
            plane(2, 6),
            plane(3),
            plane(2, 3),
            plane(2),
            plane(2),
            plane(3),
            plane(2, steps, 3),
            plane(2, steps, 3),
            plane(2, steps, 3),
            plane(2, steps, 3),
            plane(2),
            plane(2),
            plane(steps, planes + 1),
            plane(2, planes),
            plane(planes),
            plane(2, 3, 2),
            plane(2, 3, 2),
            plane(2, 3, 2),
            plane(2),
            pltpu.VMEM((rows, ny), f32),
            pltpu.VMEM((rows, ny), f32),
            pltpu.VMEM((rows, ny), f32),
            pltpu.VMEM((groups, rows, ny), f32),
            pltpu.SMEM(source_depth.shape, jnp.int32),
            pltpu.SMEM(source_column.shape, jnp.int32),
            pltpu.SMEM(wavelet.shape, f32),
            pltpu.VMEM(receiver_depth.shape, jnp.int32),
            pltpu.VMEM(receiver_column.shape, jnp.int32),
            pltpu.VMEM(traces.shape[1:], f32),
            dma((18,)),
            dma((13,)),
            dma((13,)),
            dma((2, steps, 2)),
            dma((2, steps, 2)),
            dma((2, steps, 2)),
            dma((2, steps, 2)),
            dma((2,)),
            dma((2, 5)),
            dma((2, 5)),
            dma((groups, 5)),
            dma((groups, 5)),
        ],
        compiler_params=pltpu.CompilerParams(collective_id=0, has_side_effects=True),
    )(
        wavefields,
        earth_model,
        source_depth,
        source_column,
        wavelet,
        receiver_depth,
        receiver_column,
        traces,
    )
    return summed.reshape(2, planes, nx, ny)


def solution(mesh):
    placed = (
        P(("parts", "shot"), None, None, "gz", None, None),
        P("parts", "gz", None, None),
        P(("parts", "shot")),
        P(("parts", "shot")),
        P(("parts", "shot"), None),
        P(("parts", "shot"), None),
        P(("parts", "shot"), None),
        P(("parts", "shot"), None, None),
    )
    return jax.shard_map(
        functools.partial(on_device, mesh.shape["gz"], mesh.shape["shot"]),
        mesh=mesh,
        in_specs=placed,
        out_specs=P("parts", "gz", None, None),
        check_vma=False,
    )
```

```python
import functools

import jax
import jax.numpy as jnp
from jax import lax
from jax.experimental import pallas as pl
from jax.experimental.pallas import tpu as pltpu
from jax.sharding import PartitionSpec as P

time_step = 0.15
VX, VY, VZ, SXX, SYY, SZZ, SXY, SXZ, SYZ = range(9)
MESH = pl.DeviceIdType.MESH


def kernel(
    gz_count,
    shot_count,
    wave_hbm,
    earth_hbm,
    src_depth_hbm,
    src_column_hbm,
    wavelet_hbm,
    rec_depth_hbm,
    rec_column_hbm,
    traces_hbm,
    out,
    state,
    earth,
    below,
    below_earth,
    above,
    above_earth,
    first_up,
    first_down,
    ghost_down,
    earth_last,
    earth_first,
    low_in,
    high_in,
    up_out,
    down_out,
    rest_in,
    rest_out,
    inject,
    press,
    spin,
    slope,
    grad,
    strain,
    twist,
    image,
    near_in,
    near_sum,
    cross_in,
    src_depth,
    src_column,
    wavelet,
    rec_depth,
    rec_column,
    traces,
    load_sem,
    init_send,
    init_recv,
    step_send,
    up_recv,
    down_recv,
    rest_sem,
    sum_send,
    sum_recv,
    cross_recv,
):
    planes, nx, ny = state.shape[2:]
    steps = traces.shape[0]
    last = planes - 1
    h = time_step
    gz = lax.axis_index("gz")
    shot = lax.axis_index("shot")
    has_low = gz > 0
    has_high = gz < gz_count - 1
    paired = shot_count % 2 == 0
    far = lax.rem(shot, 2) == 0

    def local(src, dst, k):
        return pltpu.make_async_copy(src, dst, load_sem.at[k])

    def loaded(dst, k):
        local(dst, dst, k).wait()

    load_first = [
        [
            local(wave_hbm.at[0, w, pl.ds(SXZ, 2), last], first_up.at[w, pl.ds(0, 2)], w),
            local(wave_hbm.at[0, w, VZ, last], first_up.at[w, 2], w),
            local(wave_hbm.at[0, w, SZZ, last], first_up.at[w, 3], w),
        ]
        for w in range(2)
    ]
    load_down = local(wave_hbm.at[0, :, SZZ, 0], first_down, 2)
    load_ghost = [
        local(wave_hbm.at[0, :, pl.ds(VX, 2), 0], ghost_down.at[:, pl.ds(0, 2)], 3),
        local(wave_hbm.at[0, :, pl.ds(SXX, 2), 0], ghost_down.at[:, pl.ds(2, 2)], 3),
        local(wave_hbm.at[0, :, SXY, 0], ghost_down.at[:, 4], 3),
    ]
    load_state = [local(wave_hbm.at[0, w], state.at[w], 4 + w) for w in range(2)]
    load_edges = [
        local(earth_hbm.at[0, last], earth_last.at[0], 6),
        local(earth_hbm.at[2, last], earth_last.at[1], 6),
    ]
    load_lowest = local(earth_hbm.at[:, 0], earth_first, 7)
    load_earth = local(earth_hbm, earth, 8)
    small = [
        local(src, dst, 9 + i)
        for i, (src, dst) in enumerate(
            (
                (traces_hbm.at[0], traces),
                (rec_depth_hbm, rec_depth),
                (rec_column_hbm, rec_column),
                (src_depth_hbm, src_depth),
                (src_column_hbm, src_column),
                (wavelet_hbm, wavelet),
            )
        )
    ]
    for copy in load_edges + load_first[0] + [load_down] + load_first[1]:
        copy.start()
    for copy in load_ghost + [load_lowest, load_state[0], load_earth] + small + [load_state[1]]:
        copy.start()

    barrier = pltpu.get_barrier_semaphore()

    @pl.when(has_low)
    def _():
        pl.semaphore_signal(barrier, inc=1, device_id={"gz": gz - 1}, device_id_type=MESH)

    @pl.when(has_high)
    def _():
        pl.semaphore_signal(barrier, inc=1, device_id={"gz": gz + 1}, device_id_type=MESH)

    for k in range(1, shot_count):
        peer = lax.rem(shot + k, shot_count)
        pl.semaphore_signal(barrier, inc=1, device_id={"shot": peer}, device_id_type=MESH)

    rows = lax.broadcasted_iota(jnp.int32, (nx, ny), 0)
    lanes = lax.broadcasted_iota(jnp.int32, (nx, ny), 1)
    cells = rows * ny + lanes

    def fx(a):
        return jnp.where(rows == nx - 1, 0.0, pltpu.roll(a, nx - 1, 0)) - a

    def bx(a):
        return a - jnp.where(rows == 0, 0.0, pltpu.roll(a, 1, 0))

    def fy(a):
        return jnp.where(lanes == ny - 1, 0.0, pltpu.roll(a, ny - 1, 1)) - a

    def by(a):
        return a - jnp.where(lanes == 0, 0.0, pltpu.roll(a, 1, 1))

    low_peers = (gz + gz_count - 1) // gz_count
    high_peers = (2 * gz_count - 2 - gz) // gz_count
    pl.semaphore_wait(barrier, low_peers + high_peers + shot_count - 1)

    def remote(src, dst, send, recv, step_to):
        return pltpu.make_async_remote_copy(
            src_ref=src,
            dst_ref=dst,
            send_sem=send,
            recv_sem=recv,
            device_id={"gz": gz + step_to},
            device_id_type=MESH,
        )

    def initial(src, dst, k, m, step_to):
        return remote(src, dst, init_send.at[m], init_recv.at[k], step_to)

    up_first = [initial(first_up.at[w, pl.ds(0, 3)], below.at[w], w, 0, 1) for w in range(2)]
    up_earth = [initial(earth_last.at[k], below_earth.at[k], 2 + k, 1, 1) for k in range(2)]
    down_first = [initial(first_down.at[w], above.at[w, 5], 4 + w, 2, -1) for w in range(2)]
    down_near = initial(earth_first.at[0], above_earth.at[0], 6, 3, -1)
    down_earth = initial(earth_first, above_earth, 6, 3, -1)
    down_far = [initial(ghost_down.at[w], above.at[w, pl.ds(0, 5)], 7 + w, 4, -1) for w in range(2)]

    loaded(earth_last, 6)
    for w in range(2):
        loaded(first_up.at[w], w)
        around = bx(first_up[w, 0]) + by(first_up[w, 1]) - first_up[w, 3]
        first_up[w, 2] = first_up[w, 2] + (h * earth_last[0]) * around

        @pl.when(has_high)
        def _(w=w):
            up_first[w].start()
            up_earth[w].start()

        if w == 0:
            load_down.wait()

        @pl.when(has_low)
        def _(w=w):
            down_first[w].start()

    load_lowest.wait()
    loaded(ghost_down, 3)

    if paired:

        @pl.when(has_low & far)
        def _():
            down_far[0].start()
            down_earth.start()

    @pl.when(jnp.logical_not(has_low))
    def _():
        below[...] = jnp.zeros_like(below)
        below_earth[...] = jnp.zeros_like(below_earth)
        low_in[...] = jnp.zeros_like(low_in)

    @pl.when(jnp.logical_not(has_high))
    def _():
        above[...] = jnp.zeros_like(above)
        above_earth[...] = jnp.zeros_like(above_earth)
        high_in[...] = jnp.zeros_like(high_in)
        rest_in[...] = jnp.zeros_like(rest_in)

    image[...] = jnp.zeros_like(image)
    load_earth.wait()
    earth[...] = earth[...] * h

    offset = gz * planes
    for copy in small:
        copy.wait()
    receivers = traces.shape[1]
    column = rec_column[...]
    depth = rec_depth[...] - offset
    row_ids = lax.broadcasted_iota(jnp.int32, (nx, receivers), 0) * ny
    past = column - row_ids
    on_row = (past >= 0) & (past < ny)
    row_hot = jnp.concatenate(
        [jnp.where(on_row & (depth == p), h, 0.0) for p in range(-1, planes)], axis=0
    )
    col_ids = lax.broadcasted_iota(jnp.int32, (ny, receivers), 0)
    col_hot = jnp.where((column & (ny - 1)) == col_ids, 1.0, 0.0)

    def fill(n, carry):
        inject[n] = lax.dot_general(
            row_hot * traces[pl.ds(n, 1), :],
            col_hot,
            (((1,), (1,)), ((), ())),
            precision=lax.Precision.HIGHEST,
            preferred_element_type=jnp.float32,
        ).reshape(planes + 1, nx, ny)
        return carry

    src_at = src_depth[0] - offset
    src_cell = src_column[0]

    def source_term(plane, n):
        cell = jnp.where(src_at == plane, src_cell, -1)
        return jnp.where(cells == cell, h * wavelet[0, n], 0.0)

    def parity(n):
        return n % 2 if isinstance(n, int) else lax.rem(n, 2)

    def mod3(n):
        return n % 3 if isinstance(n, int) else lax.rem(n, 3)

    def part_of(ref, w, n, part):
        return ref.at[w, n, pl.ds(0, 2)] if part == 0 else ref.at[w, n, 2]

    def send_up(w, n, part):
        return remote(
            part_of(up_out, w, n, part),
            part_of(low_in, w, n, part),
            step_send.at[0],
            up_recv.at[w, part, mod3(n)],
            1,
        )

    def send_down(w, n, part):
        return remote(
            part_of(down_out, w, n, part),
            part_of(high_in, w, n, part),
            step_send.at[1],
            down_recv.at[w, part, mod3(n)],
            -1,
        )

    send_rest = remote(rest_out, rest_in, rest_sem.at[0], rest_sem.at[1], -1)

    def strains(w, p, n, vx, vy, dvz, hlam, hmu):
        ex, ey = bx(vx), by(vy)
        spread = hlam * (ex + ey + dvz)
        if w == 0:
            spread = spread + source_term(p, n)
        mu2 = 2.0 * hmu
        return spread + mu2 * ex, spread + mu2 * ey, spread + mu2 * dvz

    def keep_pressure(w, p, n, total):
        at = parity(n + 1)
        if w == 0:
            press[at, p] = total * (1.0 / (3 * steps))
        else:
            image[pl.ds(p * nx, nx), :] += press[at, p] * (total * (1.0 / 3.0))

    def a_node(w, p, n):
        hb, hlam, hmu = (earth[i, p] for i in range(3))
        sxy = state[w, SXY, p]
        below_p = (below[w, i] for i in range(3)) if p == 0 else (state[w, i, p - 1] for i in (SXZ, SYZ, VZ))
        sxz_b, syz_b, vz_b = below_p
        vx = state[w, VX, p] + hb * (fx(state[w, SXX, p]) + by(sxy) + (state[w, SXZ, p] - sxz_b))
        vy = state[w, VY, p] + hb * (bx(sxy) + fy(state[w, SYY, p]) + (state[w, SYZ, p] - syz_b))
        state[w, VX, p] = vx
        state[w, VY, p] = vy
        dxx, dyy, dzz = strains(w, p, n, vx, vy, state[w, VZ, p] - vz_b, hlam, hmu)
        sxx = state[w, SXX, p] + dxx
        syy = state[w, SYY, p] + dyy
        szz = state[w, SZZ, p] + dzz
        total = sxx + syy + szz
        state[w, SXX, p] = sxx
        state[w, SYY, p] = syy
        state[w, SZZ, p] = szz
        vxy, vyx = fy(vx), fx(vy)
        state[w, SXY, p] = sxy + hmu * (vxy + vyx)
        keep_pressure(w, p, n, total)
        if w == 1:
            spin[p] = vyx - vxy

    def curl(w, p, n, vxz, vyz, vzx, vzy):
        rotation = (vzy - vyz) + (vxz - vzx) + spin[p]
        image[pl.ds((planes + p) * nx, nx), :] += press[parity(n), p] * rotation

    def b_node(w, p, n, first, upper):
        hb, hmu = earth[0, p], earth[2, p]
        vz, sxz, syz = (state[w, i, p] for i in (VZ, SXZ, SYZ))
        vx_f, vy_f, szz_f = upper
        if not first:
            vxz, vyz = vx_f - state[w, VX, p], vy_f - state[w, VY, p]
            vzx, vzy = fx(vz), fy(vz)
            sxz = sxz + hmu * (vxz + vzx)
            syz = syz + hmu * (vyz + vzy)
            state[w, SXZ, p] = sxz
            state[w, SYZ, p] = syz
            if w == 1:
                curl(w, p, n, vxz, vyz, vzx, vzy)
        term = hb * (bx(sxz) + by(syz) + (szz_f - state[w, SZZ, p]))
        if w == 1:
            term = term + inject[n, p + 1]
        vz = vz + term
        state[w, VZ, p] = vz
        return sxz, syz, vz

    def own_upper(w, p):
        return tuple(state[w, i, p + 1] for i in (VX, VY, SZZ))

    BELOW, LAST, LOWEST = range(3)
    ABOVE = 2

    def edge_at(p):
        return 0 if p == 0 else 1

    def set_slope(w, slot, vz):
        slope[w, slot, 0] = fx(vz)
        slope[w, slot, 1] = fy(vz)

    def set_grad(w, slot, sxx, syy, sxy):
        grad[w, slot, 0] = fx(sxx) + by(sxy)
        grad[w, slot, 1] = bx(sxy) + fy(syy)

    def edge_velocity(w, p):
        hb = earth[0, p]
        if p == 0:
            sxz_b, syz_b = below[w, 0], below[w, 1]
        else:
            sxz_b, syz_b = state[w, SXZ, p - 1], state[w, SYZ, p - 1]
        at = edge_at(p)
        vx = state[w, VX, p] + hb * (grad[w, at, 0] + (state[w, SXZ, p] - sxz_b))
        vy = state[w, VY, p] + hb * (grad[w, at, 1] + (state[w, SYZ, p] - syz_b))
        return vx, vy

    def edge_rise(w, p):
        return state[w, VZ, p] - (below[w, 2] if p == 0 else state[w, VZ, p - 1])

    def widen(w, at, p, n, vx, vy, hlam, hmu):
        ey = by(vy)
        strain[w, at, 1] = ey
        flat = bx(vx) + ey

        def finish(dvz):
            spread = hlam * (flat + dvz)
            if w == 0:
                spread = spread + source_term(p, n)
            strain[w, at, 0] = spread
            return spread + (2.0 * hmu) * dvz

        return finish

    def a_fast(w, p, n):
        vx, vy = edge_velocity(w, p)
        state[w, VX, p] = vx
        state[w, VY, p] = vy
        change = widen(w, edge_at(p), p, n, vx, vy, earth[1, p], earth[2, p])

        def finish():
            szz = state[w, SZZ, p] + change(edge_rise(w, p))
            state[w, SZZ, p] = szz
            return szz

        return (vx, vy), finish

    def rest_of(w, at, vx, vy, hmu, sxx, syy, sxy):
        spread, mu2 = strain[w, at, 0], 2.0 * hmu
        vxy, vyx = fy(vx), fx(vy)
        sxx = sxx + (spread + mu2 * bx(vx))
        syy = syy + (spread + mu2 * strain[w, at, 1])
        sxy = sxy + hmu * (vxy + vyx)
        set_grad(w, at, sxx, syy, sxy)
        return sxx, syy, sxy, vyx - vxy

    def a_slow(w, p, n):
        sxx, syy, sxy, turn = rest_of(
            w, edge_at(p), *(state[w, i, p] for i in (VX, VY)), earth[2, p],
            *(state[w, i, p] for i in (SXX, SYY, SXY)),
        )
        state[w, SXX, p] = sxx
        state[w, SYY, p] = syy
        state[w, SXY, p] = sxy
        keep_pressure(w, p, n, sxx + syy + state[w, SZZ, p])
        if w == 1:
            spin[p] = turn

    def a_final(w, p, n):
        vx, vy = edge_velocity(w, p)
        volume = bx(vx) + by(vy) + edge_rise(w, p)
        spread = earth[1, p] * volume
        if w == 0:
            spread = spread + source_term(p, n)
        total = state[w, SXX, p] + state[w, SYY, p] + state[w, SZZ, p]
        keep_pressure(w, p, n, total + (3.0 * spread + (2.0 * earth[2, p]) * volume))
        if w == 1:
            state[1, VX, p] = vx
            state[1, VY, p] = vy
            spin[p] = fx(vy) - fy(vx)

    def b_fast(w, p, slot, n, first, vx_f, vy_f):
        sxz, syz = state[w, SXZ, p], state[w, SYZ, p]
        if not first:
            hmu = earth[2, p]
            vxz, vyz = vx_f - state[w, VX, p], vy_f - state[w, VY, p]
            vzx, vzy = slope[w, slot, 0], slope[w, slot, 1]
            sxz = sxz + hmu * (vxz + vzx)
            syz = syz + hmu * (vyz + vzy)
            state[w, SXZ, p] = sxz
            state[w, SYZ, p] = syz
            if w == 1:
                twist[edge_at(p)] = (vzy - vyz) + (vxz - vzx)

        def flat():
            return bx(sxz) + by(syz)

        def finish(shear, szz_f):
            term = earth[0, p] * (shear + (szz_f - state[w, SZZ, p]))
            if w == 1:
                term = term + inject[n, p + 1]
            vz = state[w, VZ, p] + term
            state[w, VZ, p] = vz
            return vz

        return (sxz, syz), flat, finish

    def keep_twist(p, n):
        image[pl.ds((planes + p) * nx, nx), :] += press[parity(n), p] * (
            twist[edge_at(p)] + spin[p]
        )

    def b_below(w, n, first):
        if not first:
            hmu = below_earth[1]
            vx_m, vy_m = low_in[w, n - 1, 0], low_in[w, n - 1, 1]
            sxz = below[w, 0] + hmu * ((state[w, VX, 0] - vx_m) + slope[w, BELOW, 0])
            syz = below[w, 1] + hmu * ((state[w, VY, 0] - vy_m) + slope[w, BELOW, 1])
            below[w, 0] = sxz
            below[w, 1] = syz

        def flat():
            return None if first else bx(sxz) + by(syz)

        def finish(shear):
            szz = state[w, SZZ, 0]
            term = below_earth[0] * (szz if first else shear + (szz - low_in[w, n - 1, 2]))
            if w == 1:
                term = term + inject[n, 0]
            below[w, 2] = below[w, 2] + term

        return flat, finish

    def above_velocity(w, sxz, syz):
        hb = above_earth[0]
        vx = above[w, 0] + hb * (grad[w, ABOVE, 0] + (sxz - state[w, SXZ, last]))
        vy = above[w, 1] + hb * (grad[w, ABOVE, 1] + (syz - state[w, SYZ, last]))
        return vx, vy

    def above_fast(w, n):
        vx, vy = above_velocity(w, high_in[w, n - 1, 0], high_in[w, n - 1, 1])
        above[w, 0] = vx
        above[w, 1] = vy
        change = widen(w, ABOVE, planes, n - 1, vx, vy, above_earth[1], above_earth[2])

        def finish():
            szz = above[w, 5] + change(high_in[w, n - 1, 2] - state[w, VZ, last])
            above[w, 5] = szz
            return szz

        return (vx, vy), finish

    def above_slow(w):
        sxx, syy, sxy, _ = rest_of(
            w, ABOVE, above[w, 0], above[w, 1], above_earth[2], above[w, 2], above[w, 3], above[w, 4]
        )
        above[w, 2] = sxx
        above[w, 3] = syy
        above[w, 4] = sxy

    inner = range(1, last)
    bounds = [(nx, last * nx), ((planes + 1) * nx, (planes + last - 1) * nx)]
    early = [i for i in range(2) if bounds[i][1] > bounds[i][0]]
    bounds += [(0, nx), (last * nx, (planes + 1) * nx), ((planes + last - 1) * nx, 2 * planes * nx)]
    late = [2, 3, 4]
    pairs = shot_count // 2 if paired else shot_count

    def piece(i):
        return pl.ds(bounds[i][0], bounds[i][1] - bounds[i][0])

    def to_shot(src, dst, send, recv, target):
        return pltpu.make_async_remote_copy(
            src_ref=src,
            dst_ref=dst,
            send_sem=send,
            recv_sem=recv,
            device_id={"shot": target},
            device_id_type=MESH,
        )

    def group(i):
        return 0 if i in early else i - 1

    def gather_pair(i):
        sems = sum_send.at[0], sum_recv.at[group(i)]
        return to_shot(image.at[piece(i)], near_in.at[piece(i)], *sems, shot + 1)

    def give_back(i):
        sems = sum_send.at[1], sum_recv.at[4]
        return to_shot(out.at[piece(i)], out.at[piece(i)], *sems, shot - 1)

    def cross(i, k):
        target = lax.rem(shot + k * (shot_count // pairs), shot_count)
        sems = sum_send.at[2], cross_recv.at[k - 1, group(i)]
        return to_shot(near_sum.at[piece(i)], cross_in.at[k - 1, piece(i)], *sems, target)

    def arrived(dst, sem, which):
        count = sum(bounds[i][1] - bounds[i][0] for i in which)
        whole = dst.at[pl.ds(0, count)]
        pltpu.make_async_copy(whole, whole, sem).wait()

    def merge_pair(which):
        if paired:
            arrived(near_in, sum_recv.at[group(which[0])], which)
        for i in which:
            near_sum[piece(i), :] = image[piece(i), :]
            if paired:
                near_sum[piece(i), :] += near_in[piece(i), :]
            for k in range(1, pairs):
                cross(i, k).start()

    def merge_all(which):
        for k in range(1, pairs):
            arrived(cross_in.at[k - 1], cross_recv.at[k - 1, group(which[0])], which)
        for i in which:
            total = near_sum[piece(i), :]
            for k in range(1, pairs):
                total = total + cross_in[k - 1, piece(i), :]
            out[piece(i), :] = total
            if paired:
                give_back(i).start()

    def run(deep):
        def inside(w, n):
            for p in range(1 if deep else 0, last):
                b_node(w, p, n, isinstance(n, int) and n == 0, own_upper(w, p))
            for p in inner:
                a_node(w, p, n)

        def store(buf, values, w, n):
            for i, value in enumerate(values):
                buf[w, n, i] = value

        def start_up(w, n, part):
            @pl.when(has_high)
            def _():
                send_up(w, n, part).start()

        def start_down(w, n, part):
            @pl.when((has_low & (n < steps - 1)) if deep else has_low)
            def _():
                send_down(w, n, part).start()

        def wait_high(w, n, part):
            @pl.when(has_high)
            def _():
                send_down(w, n, part).wait_recv()

        def wait_low(w, n, part):
            @pl.when(has_low)
            def _():
                send_up(w, n, part).wait_recv()

        def first_low(w):
            @pl.when(has_low)
            def _():
                up_first[w].wait_recv()
                if w == 0:
                    up_earth[0].wait_recv()

            if w == 0:
                below_earth[0] = below_earth[0] * h

        def half(w, n, first, final):
            if first:

                @pl.when(has_high)
                def _():
                    down_first[w].wait_recv()

                szz_f = above[w, 5]
            vx_f = vy_f = None
            if final:
                for part in range(2):
                    wait_high(w, n - 1, part)
                    wait_low(w, n - 1, part)
                if deep:
                    (vx_f, vy_f), lift = above_fast(w, n)
                    szz_f = lift()
                else:
                    vx_f, vy_f, szz_f = (high_in[w, n - 1, i] for i in range(3))
                _, shear, rise = b_fast(w, last, LAST, n, first, vx_f, vy_f)
                rise(shear(), szz_f)
                shear, rise = b_below(w, n, first)
                rise(shear())
                if w == 1:
                    keep_twist(last, n)
                    if deep:
                        above_slow(w)
                a_final(w, 0, n)
                a_final(w, last, n)
            elif deep:
                if not first:
                    wait_high(w, n - 1, 0)
                    (vx_f, vy_f), lift = above_fast(w, n)
                _, shear, rise = b_fast(w, last, LAST, n, first, vx_f, vy_f)
                values, top = a_fast(w, last, n)
                store(up_out, values, w, n)
                start_up(w, n, 0)
                shear = shear()
                if not first:
                    wait_high(w, n - 1, 1)
                    szz_f = lift()
                rise(shear, szz_f)
                up_out[w, n, 2] = top()
                start_up(w, n, 1)
                if first:
                    first_low(w)
                else:
                    wait_low(w, n - 1, 0)
                shear_m, rise_m = b_below(w, n, first)
                _, bottom = a_fast(w, 0, n)
                lower = (state[w, VX, 1], state[w, VY, 1])
                values, shear, rise = b_fast(w, 0, LOWEST, n + 1, False, *lower)
                store(down_out, values, w, n + 1)
                if w == 1:

                    @pl.when(has_low & (n == steps - 2))
                    def _():
                        rest_out[...] = state[1, SXZ, 0] - state[1, SYZ, 0]
                        send_rest.start()

                start_down(w, n + 1, 0)
                shear_m, shear = shear_m(), shear()
                if not first:
                    wait_low(w, n - 1, 1)
                rise_m(shear_m)
                bottom()
                down_out[w, n + 1, 2] = rise(shear, state[w, SZZ, 1])
                start_down(w, n + 1, 1)
            else:
                if first:
                    first_low(w)
                else:
                    wait_low(w, n - 1, 0)
                    wait_high(w, n - 1, 0)
                    vx_f, vy_f = high_in[w, n - 1, 0], high_in[w, n - 1, 1]
                shear_m, rise_m = b_below(w, n, first)
                _, shear, rise = b_fast(w, last, LAST, n, first, vx_f, vy_f)
                values, bottom = a_fast(w, 0, n)
                store(down_out, values, w, n)
                values, top = a_fast(w, last, n)
                store(up_out, values, w, n)
                start_down(w, n, 0)
                start_up(w, n, 0)
                shear_m, shear = shear_m(), shear()
                if not first:
                    wait_low(w, n - 1, 1)
                    wait_high(w, n - 1, 1)
                    szz_f = high_in[w, n - 1, 2]
                rise_m(shear_m)
                rise(shear, szz_f)
                down_out[w, n, 2] = bottom()
                up_out[w, n, 2] = top()
                start_down(w, n, 1)
                start_up(w, n, 1)

            if not final:
                if w == 1 and not first:
                    keep_twist(last, n)
                a_slow(w, 0, n)
                a_slow(w, last, n)
                if deep:
                    if not first:
                        above_slow(w)
                    if w == 1:
                        keep_twist(0, n + 1)
                    set_slope(w, LOWEST, state[w, VZ, 0])
                set_slope(w, BELOW, below[w, 2])
                set_slope(w, LAST, state[w, VZ, last])
                inside(w, n + 1)
                if w == 1 and not deep:

                    @pl.when(has_low & (n == steps - 2))
                    def _():
                        shear = state[1, SXZ, 0] - state[1, SYZ, 0]
                        slide = grad[1, 0, 0] - grad[1, 0, 1] + shear
                        rest_out[...] = state[1, VX, 0] - state[1, VY, 0] + earth[0, 0] * slide
                        send_rest.start()

            elif w == 1:

                @pl.when(has_high)
                def _():
                    if not deep:
                        down_near.wait_recv()
                    send_rest.wait_recv()

                shear = state[1, SXZ, last] - state[1, SYZ, last]
                if deep:
                    slide = grad[1, ABOVE, 0] - grad[1, ABOVE, 1] + (rest_in[...] - shear)
                    gap = above[1, 0] - above[1, 1] + above_earth[0] * slide
                else:
                    gap = rest_in[...] - (above_earth[0] * h) * shear
                for p in range(planes):
                    if 0 < p < last - 1:
                        continue
                    vx, vy, vz = (state[1, i, p] for i in (VX, VY, VZ))
                    if p == last:
                        turn = gap - (vx - vy), 0.0
                    else:
                        turn = state[1, VX, p + 1] - vx, state[1, VY, p + 1] - vy
                    curl(1, p, n + 1, *turn, fx(vz), fy(vz))

        for w in range(2):
            load_state[w].wait()
            if w == 1:
                if deep:

                    @pl.when(has_low)
                    def _():
                        down_far[1].start()

                fill(0, 0)
            if deep:
                values, shear, rise = b_fast(w, 0, LOWEST, 0, True, None, None)
                store(down_out, values, w, 0)
                start_down(w, 0, 0)
                down_out[w, 0, 2] = rise(shear(), state[w, SZZ, 1])
                start_down(w, 0, 1)
                set_slope(w, LOWEST, state[w, VZ, 0])
            for p in sorted({0, last}):
                set_grad(w, edge_at(p), *(state[w, i, p] for i in (SXX, SYY, SXY)))
            inside(w, 0)
        lax.fori_loop(1, steps, fill, 0)
        for w in range(2):
            half(w, 0, True, False)

        @pl.when(has_low)
        def _():
            up_earth[1].wait_recv()

        below_earth[1] = below_earth[1] * h

        def take_ghost(w):
            @pl.when(has_high)
            def _():
                down_far[w].wait_recv()

            set_grad(w, ABOVE, above[w, 2], above[w, 3], above[w, 4])

        if deep:

            @pl.when(has_high)
            def _():
                down_earth.wait_recv()

            for i in range(3):
                above_earth[i] = above_earth[i] * h
            take_ghost(0)
            if steps == 2:
                take_ghost(1)
        else:

            @pl.when(has_low)
            def _():
                down_near.start()

        def body(n, carry):
            half(0, n, False, False)
            if deep:
                pl.when(n == 1)(lambda: take_ghost(1))
            half(1, n, False, False)
            return carry

        lax.fori_loop(1, steps - 1, body, 0)
        for p in range(1, last - 1):
            vx, vy, vz = (state[1, i, p] for i in (VX, VY, VZ))
            curl(1, p, steps, state[1, VX, p + 1] - vx, state[1, VY, p + 1] - vy, fx(vz), fy(vz))
        if deep:
            for i in early:
                gather_pair(i).start()
        half(0, steps - 1, False, True)
        if not deep:
            merge_pair(early)
        half(1, steps - 1, False, True)
        if deep:
            for i in late:
                gather_pair(i).start()
            arrived(out, sum_recv.at[4], early + late)
            arrived(image, sum_send.at[0], early + late)
        else:
            for i in late:
                merge_pair([i])
            for which in [early] + [[i] for i in late]:
                merge_all(which)
            for k in range(1, pairs):
                arrived(near_sum, sum_send.at[2], early + late)
            if paired:
                arrived(out, sum_send.at[1], early + late)

    if paired:
        pl.when(far)(lambda: run(True))
        pl.when(jnp.logical_not(far))(lambda: run(False))
    else:
        run(False)

    def left(src, sem):
        pltpu.make_async_copy(src, src, sem).wait()

    @pl.when(has_high)
    def _():
        left(below, init_send.at[0])
        left(earth_last, init_send.at[1])
        left(up_out.at[:, pl.ds(0, steps - 1)], step_send.at[0])

    def drain_near():
        @pl.when(has_low)
        def _():
            down_near.wait_send()

    def drain_far():
        @pl.when(has_low)
        def _():
            left(ghost_down, init_send.at[4])
            down_earth.wait_send()

    if paired:
        pl.when(far)(drain_far)
        pl.when(jnp.logical_not(far))(drain_near)
    else:
        drain_near()

    @pl.when(has_low)
    def _():
        left(first_down, init_send.at[2])
        send_rest.wait_send()
        left(down_out.at[:, pl.ds(0, steps - 1)], step_send.at[1])


def on_device(
    gz_count,
    shot_count,
    wavefields,
    earth_model,
    source_depth,
    source_column,
    wavelet,
    receiver_depth,
    receiver_column,
    traces,
):
    planes, nx, ny = wavefields.shape[3:]
    steps = wavelet.shape[1]
    rows = 2 * planes * nx
    groups = max((shot_count + 1) // 2 - 1, 1)
    f32 = jnp.float32
    vmem = pl.BlockSpec(memory_space=pltpu.VMEM)
    hbm = pl.BlockSpec(memory_space=pltpu.HBM)
    dma = pltpu.SemaphoreType.DMA

    def plane(*lead):
        return pltpu.VMEM((*lead, nx, ny), f32)

    summed = pl.pallas_call(
        functools.partial(kernel, gz_count, shot_count),
        out_shape=pltpu.VMEM((rows, ny), f32),
        in_specs=[hbm] * 8,
        out_specs=vmem,
        scratch_shapes=[
            plane(2, 9, planes),
            plane(3, planes),
            plane(2, 3),
            plane(2),
            plane(2, 6),
            plane(3),
            plane(2, 4),
            plane(2),
            plane(2, 5),
            plane(2),
            plane(3),
            plane(2, steps, 3),
            plane(2, steps, 3),
            plane(2, steps, 3),
            plane(2, steps, 3),
            plane(),
            plane(),
            plane(steps, planes + 1),
            plane(2, planes),
            plane(planes),
            plane(2, 3, 2),
            plane(2, 3, 2),
            plane(2, 3, 2),
            plane(2),
            pltpu.VMEM((rows, ny), f32),
            pltpu.VMEM((rows, ny), f32),
            pltpu.VMEM((rows, ny), f32),
            pltpu.VMEM((groups, rows, ny), f32),
            pltpu.SMEM(source_depth.shape, jnp.int32),
            pltpu.SMEM(source_column.shape, jnp.int32),
            pltpu.SMEM(wavelet.shape, f32),
            pltpu.VMEM(receiver_depth.shape, jnp.int32),
            pltpu.VMEM(receiver_column.shape, jnp.int32),
            pltpu.VMEM(traces.shape[1:], f32),
            dma((15,)),
            dma((5,)),
            dma((9,)),
            dma((2,)),
            dma((2, 2, 3)),
            dma((2, 2, 3)),
            dma((2,)),
            dma((3,)),
            dma((5,)),
            dma((groups, 4)),
        ],
        compiler_params=pltpu.CompilerParams(collective_id=0, has_side_effects=True),
    )(
        wavefields,
        earth_model,
        source_depth,
        source_column,
        wavelet,
        receiver_depth,
        receiver_column,
        traces,
    )
    return summed.reshape(2, planes, nx, ny)


def solution(mesh):
    placed = (
        P(("parts", "shot"), None, None, "gz", None, None),
        P("parts", "gz", None, None),
        P(("parts", "shot")),
        P(("parts", "shot")),
        P(("parts", "shot"), None),
        P(("parts", "shot"), None),
        P(("parts", "shot"), None),
        P(("parts", "shot"), None, None),
    )
    return jax.shard_map(
        functools.partial(on_device, mesh.shape["gz"], mesh.shape["shot"]),
        mesh=mesh,
        in_specs=placed,
        out_specs=P("parts", "gz", None, None),
        check_vma=False,
    )
```

```python
import functools

import jax
import jax.numpy as jnp
from jax import lax
from jax.experimental import pallas as pl
from jax.experimental.pallas import tpu as pltpu
from jax.sharding import PartitionSpec as P

time_step = 0.15
VX, VY, VZ, SXX, SYY, SZZ, SXY, SXZ, SYZ = range(9)
MESH = pl.DeviceIdType.MESH


def kernel(
    gz_count,
    shot_count,
    wave_hbm,
    earth_hbm,
    src_depth_hbm,
    src_column_hbm,
    wavelet_hbm,
    rec_depth_hbm,
    rec_column_hbm,
    traces_hbm,
    out,
    state,
    earth,
    below,
    below_earth,
    above,
    above_earth,
    first_up,
    first_down,
    ghost_down,
    earth_last,
    earth_first,
    low_in,
    high_in,
    up_out,
    down_out,
    rest_in,
    rest_out,
    inject,
    press,
    spin,
    slope,
    grad,
    strain,
    twist,
    image,
    near_in,
    near_sum,
    cross_in,
    src_depth,
    src_column,
    wavelet,
    rec_depth,
    rec_column,
    traces,
    load_sem,
    init_send,
    init_recv,
    step_send,
    up_recv,
    down_recv,
    rest_sem,
    sum_send,
    sum_recv,
    cross_recv,
):
    planes, nx, ny = state.shape[2:]
    steps = traces.shape[0]
    last = planes - 1
    h = time_step
    gz = lax.axis_index("gz")
    shot = lax.axis_index("shot")
    has_low = gz > 0
    has_high = gz < gz_count - 1
    paired = shot_count % 2 == 0
    far = lax.rem(shot, 2) == 0

    def local(src, dst, k):
        return pltpu.make_async_copy(src, dst, load_sem.at[k])

    def loaded(dst, k):
        local(dst, dst, k).wait()

    load_first = [
        [
            local(wave_hbm.at[0, w, pl.ds(SXZ, 2), last], first_up.at[w, pl.ds(0, 2)], w),
            local(wave_hbm.at[0, w, VZ, last], first_up.at[w, 2], w),
            local(wave_hbm.at[0, w, SZZ, last], first_up.at[w, 3], w),
        ]
        for w in range(2)
    ]
    load_down = local(wave_hbm.at[0, :, SZZ, 0], first_down, 2)
    load_ghost = [
        local(wave_hbm.at[0, :, pl.ds(VX, 2), 0], ghost_down.at[:, pl.ds(0, 2)], 3),
        local(wave_hbm.at[0, :, pl.ds(SXX, 2), 0], ghost_down.at[:, pl.ds(2, 2)], 3),
        local(wave_hbm.at[0, :, SXY, 0], ghost_down.at[:, 4], 3),
    ]
    load_state = [local(wave_hbm.at[0, w], state.at[w], 4 + w) for w in range(2)]
    load_edges = [
        local(earth_hbm.at[0, last], earth_last.at[0], 6),
        local(earth_hbm.at[2, last], earth_last.at[1], 6),
    ]
    load_lowest = local(earth_hbm.at[:, 0], earth_first, 7)
    load_earth = local(earth_hbm, earth, 8)
    small = [
        local(src, dst, 9 + i)
        for i, (src, dst) in enumerate(
            (
                (traces_hbm.at[0], traces),
                (rec_depth_hbm, rec_depth),
                (rec_column_hbm, rec_column),
                (src_depth_hbm, src_depth),
                (src_column_hbm, src_column),
                (wavelet_hbm, wavelet),
            )
        )
    ]
    for copy in load_edges + load_first[0] + [load_down] + load_first[1]:
        copy.start()
    for copy in load_ghost + [load_lowest, load_state[0], load_earth] + small + [load_state[1]]:
        copy.start()

    barrier = pltpu.get_barrier_semaphore()

    @pl.when(has_low)
    def _():
        pl.semaphore_signal(barrier, inc=1, device_id={"gz": gz - 1}, device_id_type=MESH)

    @pl.when(has_high)
    def _():
        pl.semaphore_signal(barrier, inc=1, device_id={"gz": gz + 1}, device_id_type=MESH)

    for k in range(1, shot_count):
        peer = lax.rem(shot + k, shot_count)
        pl.semaphore_signal(barrier, inc=1, device_id={"shot": peer}, device_id_type=MESH)

    rows = lax.broadcasted_iota(jnp.int32, (nx, ny), 0)
    lanes = lax.broadcasted_iota(jnp.int32, (nx, ny), 1)
    cells = rows * ny + lanes

    def fx(a):
        return jnp.where(rows == nx - 1, 0.0, pltpu.roll(a, nx - 1, 0)) - a

    def bx(a):
        return a - jnp.where(rows == 0, 0.0, pltpu.roll(a, 1, 0))

    def fy(a):
        return jnp.where(lanes == ny - 1, 0.0, pltpu.roll(a, ny - 1, 1)) - a

    def by(a):
        return a - jnp.where(lanes == 0, 0.0, pltpu.roll(a, 1, 1))

    low_peers = (gz + gz_count - 1) // gz_count
    high_peers = (2 * gz_count - 2 - gz) // gz_count
    pl.semaphore_wait(barrier, low_peers + high_peers + shot_count - 1)

    def remote(src, dst, send, recv, step_to):
        return pltpu.make_async_remote_copy(
            src_ref=src,
            dst_ref=dst,
            send_sem=send,
            recv_sem=recv,
            device_id={"gz": gz + step_to},
            device_id_type=MESH,
        )

    def initial(src, dst, k, m, step_to):
        return remote(src, dst, init_send.at[m], init_recv.at[k], step_to)

    up_first = [initial(first_up.at[w, pl.ds(0, 3)], below.at[w], w, 0, 1) for w in range(2)]
    up_earth = [initial(earth_last.at[k], below_earth.at[k], 2 + k, 1, 1) for k in range(2)]
    down_first = [initial(first_down.at[w], above.at[w, 5], 4 + w, 2, -1) for w in range(2)]
    if paired:
        share_near = pltpu.make_async_remote_copy(
            src_ref=above_earth.at[0],
            dst_ref=above_earth.at[0],
            send_sem=init_send.at[5],
            recv_sem=init_recv.at[6],
            device_id={"shot": shot + 1},
            device_id_type=MESH,
        )
    else:
        down_near = initial(earth_first.at[0], above_earth.at[0], 6, 3, -1)
    down_earth = initial(earth_first, above_earth, 6, 3, -1)
    down_far = [initial(ghost_down.at[w], above.at[w, pl.ds(0, 5)], 7 + w, 4, -1) for w in range(2)]

    loaded(earth_last, 6)
    for w in range(2):
        loaded(first_up.at[w], w)
        around = bx(first_up[w, 0]) + by(first_up[w, 1]) - first_up[w, 3]
        first_up[w, 2] = first_up[w, 2] + (h * earth_last[0]) * around

        @pl.when(has_high)
        def _(w=w):
            up_first[w].start()
            up_earth[w].start()

        if w == 0:
            load_down.wait()

        @pl.when(has_low)
        def _(w=w):
            down_first[w].start()

    load_lowest.wait()
    loaded(ghost_down, 3)

    if paired:

        @pl.when(has_low & far)
        def _():
            down_far[0].start()
            down_earth.start()

    @pl.when(jnp.logical_not(has_low))
    def _():
        below[...] = jnp.zeros_like(below)
        below_earth[...] = jnp.zeros_like(below_earth)
        low_in[...] = jnp.zeros_like(low_in)

    @pl.when(jnp.logical_not(has_high))
    def _():
        above[...] = jnp.zeros_like(above)
        above_earth[...] = jnp.zeros_like(above_earth)
        high_in[...] = jnp.zeros_like(high_in)
        rest_in[...] = jnp.zeros_like(rest_in)

    image[...] = jnp.zeros_like(image)
    load_earth.wait()
    earth[...] = earth[...] * h

    offset = gz * planes
    for copy in small:
        copy.wait()
    receivers = traces.shape[1]
    column = rec_column[...]
    depth = rec_depth[...] - offset
    row_ids = lax.broadcasted_iota(jnp.int32, (nx, receivers), 0) * ny
    past = column - row_ids
    on_row = (past >= 0) & (past < ny)
    row_hot = jnp.concatenate(
        [jnp.where(on_row & (depth == p), h, 0.0) for p in range(-1, planes)], axis=0
    )
    col_ids = lax.broadcasted_iota(jnp.int32, (ny, receivers), 0)
    col_hot = jnp.where((column & (ny - 1)) == col_ids, 1.0, 0.0)

    def fill(n, carry):
        inject[n] = lax.dot_general(
            row_hot * traces[pl.ds(n, 1), :],
            col_hot,
            (((1,), (1,)), ((), ())),
            precision=lax.Precision.HIGHEST,
            preferred_element_type=jnp.float32,
        ).reshape(planes + 1, nx, ny)
        return carry

    src_at = src_depth[0] - offset
    src_cell = src_column[0]

    def source_term(plane, n):
        cell = jnp.where(src_at == plane, src_cell, -1)
        return jnp.where(cells == cell, h * wavelet[0, n], 0.0)

    def parity(n):
        return n % 2 if isinstance(n, int) else lax.rem(n, 2)

    def mod3(n):
        return n % 3 if isinstance(n, int) else lax.rem(n, 3)

    def part_of(ref, w, n, part):
        return ref.at[w, n, pl.ds(0, 2)] if part == 0 else ref.at[w, n, 2]

    def send_up(w, n, part):
        return remote(
            part_of(up_out, w, n, part),
            part_of(low_in, w, n, part),
            step_send.at[0],
            up_recv.at[w, part, mod3(n)],
            1,
        )

    def send_down(w, n, part):
        return remote(
            part_of(down_out, w, n, part),
            part_of(high_in, w, n, part),
            step_send.at[1],
            down_recv.at[w, part, mod3(n)],
            -1,
        )

    send_rest = remote(rest_out, rest_in, rest_sem.at[0], rest_sem.at[1], -1)

    def strains(w, p, n, vx, vy, dvz, hlam, hmu):
        ex, ey = bx(vx), by(vy)
        spread = hlam * (ex + ey + dvz)
        if w == 0:
            spread = spread + source_term(p, n)
        mu2 = 2.0 * hmu
        return spread + mu2 * ex, spread + mu2 * ey, spread + mu2 * dvz

    def keep_pressure(w, p, n, total):
        at = parity(n + 1)
        if w == 0:
            press[at, p] = total * (1.0 / (3 * steps))
        else:
            image[pl.ds(p * nx, nx), :] += press[at, p] * (total * (1.0 / 3.0))

    def a_node(w, p, n):
        hb, hlam, hmu = (earth[i, p] for i in range(3))
        sxy = state[w, SXY, p]
        below_p = (below[w, i] for i in range(3)) if p == 0 else (state[w, i, p - 1] for i in (SXZ, SYZ, VZ))
        sxz_b, syz_b, vz_b = below_p
        vx = state[w, VX, p] + hb * (fx(state[w, SXX, p]) + by(sxy) + (state[w, SXZ, p] - sxz_b))
        vy = state[w, VY, p] + hb * (bx(sxy) + fy(state[w, SYY, p]) + (state[w, SYZ, p] - syz_b))
        state[w, VX, p] = vx
        state[w, VY, p] = vy
        dxx, dyy, dzz = strains(w, p, n, vx, vy, state[w, VZ, p] - vz_b, hlam, hmu)
        sxx = state[w, SXX, p] + dxx
        syy = state[w, SYY, p] + dyy
        szz = state[w, SZZ, p] + dzz
        total = sxx + syy + szz
        state[w, SXX, p] = sxx
        state[w, SYY, p] = syy
        state[w, SZZ, p] = szz
        vxy, vyx = fy(vx), fx(vy)
        state[w, SXY, p] = sxy + hmu * (vxy + vyx)
        keep_pressure(w, p, n, total)
        if w == 1:
            spin[p] = vyx - vxy

    def curl(w, p, n, vxz, vyz, vzx, vzy):
        rotation = (vzy - vyz) + (vxz - vzx) + spin[p]
        image[pl.ds((planes + p) * nx, nx), :] += press[parity(n), p] * rotation

    def b_node(w, p, n, first, upper):
        hb, hmu = earth[0, p], earth[2, p]
        vz, sxz, syz = (state[w, i, p] for i in (VZ, SXZ, SYZ))
        vx_f, vy_f, szz_f = upper
        if not first:
            vxz, vyz = vx_f - state[w, VX, p], vy_f - state[w, VY, p]
            vzx, vzy = fx(vz), fy(vz)
            sxz = sxz + hmu * (vxz + vzx)
            syz = syz + hmu * (vyz + vzy)
            state[w, SXZ, p] = sxz
            state[w, SYZ, p] = syz
            if w == 1:
                curl(w, p, n, vxz, vyz, vzx, vzy)
        term = hb * (bx(sxz) + by(syz) + (szz_f - state[w, SZZ, p]))
        if w == 1:
            term = term + inject[n, p + 1]
        vz = vz + term
        state[w, VZ, p] = vz
        return sxz, syz, vz

    def own_upper(w, p):
        return tuple(state[w, i, p + 1] for i in (VX, VY, SZZ))

    BELOW, LAST, LOWEST = range(3)
    ABOVE = 2

    def edge_at(p):
        return 0 if p == 0 else 1

    def set_slope(w, slot, vz):
        slope[w, slot, 0] = fx(vz)
        slope[w, slot, 1] = fy(vz)

    def set_grad(w, slot, sxx, syy, sxy):
        grad[w, slot, 0] = fx(sxx) + by(sxy)
        grad[w, slot, 1] = bx(sxy) + fy(syy)

    def edge_velocity(w, p):
        hb = earth[0, p]
        if p == 0:
            sxz_b, syz_b = below[w, 0], below[w, 1]
        else:
            sxz_b, syz_b = state[w, SXZ, p - 1], state[w, SYZ, p - 1]
        at = edge_at(p)
        vx = state[w, VX, p] + hb * (grad[w, at, 0] + (state[w, SXZ, p] - sxz_b))
        vy = state[w, VY, p] + hb * (grad[w, at, 1] + (state[w, SYZ, p] - syz_b))
        return vx, vy

    def edge_rise(w, p):
        return state[w, VZ, p] - (below[w, 2] if p == 0 else state[w, VZ, p - 1])

    def widen(w, at, p, n, vx, vy, hlam, hmu):
        ey = by(vy)
        strain[w, at, 1] = ey
        flat = bx(vx) + ey

        def finish(dvz):
            spread = hlam * (flat + dvz)
            if w == 0:
                spread = spread + source_term(p, n)
            strain[w, at, 0] = spread
            return spread + (2.0 * hmu) * dvz

        return finish

    def a_fast(w, p, n):
        vx, vy = edge_velocity(w, p)
        state[w, VX, p] = vx
        state[w, VY, p] = vy
        change = widen(w, edge_at(p), p, n, vx, vy, earth[1, p], earth[2, p])

        def finish():
            szz = state[w, SZZ, p] + change(edge_rise(w, p))
            state[w, SZZ, p] = szz
            return szz

        return (vx, vy), finish

    def rest_of(w, at, vx, vy, hmu, sxx, syy, sxy):
        spread, mu2 = strain[w, at, 0], 2.0 * hmu
        vxy, vyx = fy(vx), fx(vy)
        sxx = sxx + (spread + mu2 * bx(vx))
        syy = syy + (spread + mu2 * strain[w, at, 1])
        sxy = sxy + hmu * (vxy + vyx)
        set_grad(w, at, sxx, syy, sxy)
        return sxx, syy, sxy, vyx - vxy

    def a_slow(w, p, n):
        sxx, syy, sxy, turn = rest_of(
            w, edge_at(p), *(state[w, i, p] for i in (VX, VY)), earth[2, p],
            *(state[w, i, p] for i in (SXX, SYY, SXY)),
        )
        state[w, SXX, p] = sxx
        state[w, SYY, p] = syy
        state[w, SXY, p] = sxy
        keep_pressure(w, p, n, sxx + syy + state[w, SZZ, p])
        if w == 1:
            spin[p] = turn

    def a_final(w, p, n):
        vx, vy = edge_velocity(w, p)
        volume = bx(vx) + by(vy) + edge_rise(w, p)
        spread = earth[1, p] * volume
        if w == 0:
            spread = spread + source_term(p, n)
        total = state[w, SXX, p] + state[w, SYY, p] + state[w, SZZ, p]
        keep_pressure(w, p, n, total + (3.0 * spread + (2.0 * earth[2, p]) * volume))
        if w == 1:
            state[1, VX, p] = vx
            state[1, VY, p] = vy
            spin[p] = fx(vy) - fy(vx)

    def b_fast(w, p, slot, n, first, vx_f, vy_f):
        sxz, syz = state[w, SXZ, p], state[w, SYZ, p]
        if not first:
            hmu = earth[2, p]
            vxz, vyz = vx_f - state[w, VX, p], vy_f - state[w, VY, p]
            vzx, vzy = slope[w, slot, 0], slope[w, slot, 1]
            sxz = sxz + hmu * (vxz + vzx)
            syz = syz + hmu * (vyz + vzy)
            state[w, SXZ, p] = sxz
            state[w, SYZ, p] = syz
            if w == 1:
                twist[edge_at(p)] = (vzy - vyz) + (vxz - vzx)

        def flat():
            return bx(sxz) + by(syz)

        def finish(shear, szz_f):
            term = earth[0, p] * (shear + (szz_f - state[w, SZZ, p]))
            if w == 1:
                term = term + inject[n, p + 1]
            vz = state[w, VZ, p] + term
            state[w, VZ, p] = vz
            return vz

        return (sxz, syz), flat, finish

    def keep_twist(p, n):
        image[pl.ds((planes + p) * nx, nx), :] += press[parity(n), p] * (
            twist[edge_at(p)] + spin[p]
        )

    def b_below(w, n, first):
        if not first:
            hmu = below_earth[1]
            vx_m, vy_m = low_in[w, n - 1, 0], low_in[w, n - 1, 1]
            sxz = below[w, 0] + hmu * ((state[w, VX, 0] - vx_m) + slope[w, BELOW, 0])
            syz = below[w, 1] + hmu * ((state[w, VY, 0] - vy_m) + slope[w, BELOW, 1])
            below[w, 0] = sxz
            below[w, 1] = syz

        def flat():
            return None if first else bx(sxz) + by(syz)

        def finish(shear):
            szz = state[w, SZZ, 0]
            term = below_earth[0] * (szz if first else shear + (szz - low_in[w, n - 1, 2]))
            if w == 1:
                term = term + inject[n, 0]
            below[w, 2] = below[w, 2] + term

        return flat, finish

    def above_velocity(w, sxz, syz):
        hb = above_earth[0]
        vx = above[w, 0] + hb * (grad[w, ABOVE, 0] + (sxz - state[w, SXZ, last]))
        vy = above[w, 1] + hb * (grad[w, ABOVE, 1] + (syz - state[w, SYZ, last]))
        return vx, vy

    def above_fast(w, n):
        vx, vy = above_velocity(w, high_in[w, n - 1, 0], high_in[w, n - 1, 1])
        above[w, 0] = vx
        above[w, 1] = vy
        change = widen(w, ABOVE, planes, n - 1, vx, vy, above_earth[1], above_earth[2])

        def finish():
            szz = above[w, 5] + change(high_in[w, n - 1, 2] - state[w, VZ, last])
            above[w, 5] = szz
            return szz

        return (vx, vy), finish

    def above_slow(w):
        sxx, syy, sxy, _ = rest_of(
            w, ABOVE, above[w, 0], above[w, 1], above_earth[2], above[w, 2], above[w, 3], above[w, 4]
        )
        above[w, 2] = sxx
        above[w, 3] = syy
        above[w, 4] = sxy

    inner = range(1, last)
    bounds = [(nx, last * nx), ((planes + 1) * nx, (planes + last - 1) * nx)]
    early = [i for i in range(2) if bounds[i][1] > bounds[i][0]]
    bounds += [(0, nx), (last * nx, (planes + 1) * nx), ((planes + last - 1) * nx, 2 * planes * nx)]
    late = [2, 3, 4]
    pairs = shot_count // 2 if paired else shot_count

    def piece(i):
        return pl.ds(bounds[i][0], bounds[i][1] - bounds[i][0])

    def to_shot(src, dst, send, recv, target):
        return pltpu.make_async_remote_copy(
            src_ref=src,
            dst_ref=dst,
            send_sem=send,
            recv_sem=recv,
            device_id={"shot": target},
            device_id_type=MESH,
        )

    def group(i):
        return 0 if i in early else i - 1

    def gather_pair(i):
        sems = sum_send.at[0], sum_recv.at[group(i)]
        return to_shot(image.at[piece(i)], near_in.at[piece(i)], *sems, shot + 1)

    def give_back(i):
        sems = sum_send.at[1], sum_recv.at[4]
        return to_shot(out.at[piece(i)], out.at[piece(i)], *sems, shot - 1)

    def cross(i, k):
        target = lax.rem(shot + k * (shot_count // pairs), shot_count)
        sems = sum_send.at[2], cross_recv.at[k - 1, group(i)]
        return to_shot(near_sum.at[piece(i)], cross_in.at[k - 1, piece(i)], *sems, target)

    def arrived(dst, sem, which):
        count = sum(bounds[i][1] - bounds[i][0] for i in which)
        whole = dst.at[pl.ds(0, count)]
        pltpu.make_async_copy(whole, whole, sem).wait()

    def merge_pair(which):
        if paired:
            arrived(near_in, sum_recv.at[group(which[0])], which)
        for i in which:
            near_sum[piece(i), :] = image[piece(i), :]
            if paired:
                near_sum[piece(i), :] += near_in[piece(i), :]
            for k in range(1, pairs):
                cross(i, k).start()

    def merge_all(which):
        for k in range(1, pairs):
            arrived(cross_in.at[k - 1], cross_recv.at[k - 1, group(which[0])], which)
        for i in which:
            total = near_sum[piece(i), :]
            for k in range(1, pairs):
                total = total + cross_in[k - 1, piece(i), :]
            out[piece(i), :] = total
            if paired:
                give_back(i).start()

    def run(deep):
        def inside(w, n):
            for p in range(1 if deep else 0, last):
                b_node(w, p, n, isinstance(n, int) and n == 0, own_upper(w, p))
            for p in inner:
                a_node(w, p, n)

        def store(buf, values, w, n):
            for i, value in enumerate(values):
                buf[w, n, i] = value

        def start_up(w, n, part):
            @pl.when(has_high)
            def _():
                send_up(w, n, part).start()

        def start_down(w, n, part):
            @pl.when((has_low & (n < steps - 1)) if deep else has_low)
            def _():
                send_down(w, n, part).start()

        def wait_high(w, n, part):
            @pl.when(has_high)
            def _():
                send_down(w, n, part).wait_recv()

        def wait_low(w, n, part):
            @pl.when(has_low)
            def _():
                send_up(w, n, part).wait_recv()

        def first_low(w):
            @pl.when(has_low)
            def _():
                up_first[w].wait_recv()
                if w == 0:
                    up_earth[0].wait_recv()

            if w == 0:
                below_earth[0] = below_earth[0] * h

        def half(w, n, first, final):
            if first:

                @pl.when(has_high)
                def _():
                    down_first[w].wait_recv()

                szz_f = above[w, 5]
            vx_f = vy_f = None
            if final:
                for part in range(2):
                    wait_high(w, n - 1, part)
                    wait_low(w, n - 1, part)
                if deep:
                    (vx_f, vy_f), lift = above_fast(w, n)
                    szz_f = lift()
                else:
                    vx_f, vy_f, szz_f = (high_in[w, n - 1, i] for i in range(3))
                _, shear, rise = b_fast(w, last, LAST, n, first, vx_f, vy_f)
                rise(shear(), szz_f)
                shear, rise = b_below(w, n, first)
                rise(shear())
                if w == 1:
                    keep_twist(last, n)
                    if deep:
                        above_slow(w)
                a_final(w, 0, n)
                a_final(w, last, n)
            elif deep:
                if not first:
                    wait_high(w, n - 1, 0)
                    (vx_f, vy_f), lift = above_fast(w, n)
                _, shear, rise = b_fast(w, last, LAST, n, first, vx_f, vy_f)
                values, top = a_fast(w, last, n)
                store(up_out, values, w, n)
                start_up(w, n, 0)
                shear = shear()
                if not first:
                    wait_high(w, n - 1, 1)
                    szz_f = lift()
                rise(shear, szz_f)
                up_out[w, n, 2] = top()
                start_up(w, n, 1)
                if first:
                    first_low(w)
                else:
                    wait_low(w, n - 1, 0)
                shear_m, rise_m = b_below(w, n, first)
                _, bottom = a_fast(w, 0, n)
                lower = (state[w, VX, 1], state[w, VY, 1])
                values, shear, rise = b_fast(w, 0, LOWEST, n + 1, False, *lower)
                store(down_out, values, w, n + 1)
                if w == 1:

                    @pl.when(has_low & (n == steps - 2))
                    def _():
                        rest_out[...] = state[1, SXZ, 0] - state[1, SYZ, 0]
                        send_rest.start()

                start_down(w, n + 1, 0)
                shear_m, shear = shear_m(), shear()
                if not first:
                    wait_low(w, n - 1, 1)
                rise_m(shear_m)
                bottom()
                down_out[w, n + 1, 2] = rise(shear, state[w, SZZ, 1])
                start_down(w, n + 1, 1)
            else:
                if first:
                    first_low(w)
                else:
                    wait_low(w, n - 1, 0)
                    wait_high(w, n - 1, 0)
                    vx_f, vy_f = high_in[w, n - 1, 0], high_in[w, n - 1, 1]
                shear_m, rise_m = b_below(w, n, first)
                _, shear, rise = b_fast(w, last, LAST, n, first, vx_f, vy_f)
                values, bottom = a_fast(w, 0, n)
                store(down_out, values, w, n)
                values, top = a_fast(w, last, n)
                store(up_out, values, w, n)
                start_down(w, n, 0)
                start_up(w, n, 0)
                shear_m, shear = shear_m(), shear()
                if not first:
                    wait_low(w, n - 1, 1)
                    wait_high(w, n - 1, 1)
                    szz_f = high_in[w, n - 1, 2]
                rise_m(shear_m)
                rise(shear, szz_f)
                down_out[w, n, 2] = bottom()
                up_out[w, n, 2] = top()
                start_down(w, n, 1)
                start_up(w, n, 1)

            if not final:
                if w == 1 and not first:
                    keep_twist(last, n)
                a_slow(w, 0, n)
                a_slow(w, last, n)
                if deep:
                    if not first:
                        above_slow(w)
                    if w == 1:
                        keep_twist(0, n + 1)
                    set_slope(w, LOWEST, state[w, VZ, 0])
                set_slope(w, BELOW, below[w, 2])
                set_slope(w, LAST, state[w, VZ, last])
                inside(w, n + 1)
                if w == 1 and not deep:

                    @pl.when(has_low & (n == steps - 2))
                    def _():
                        shear = state[1, SXZ, 0] - state[1, SYZ, 0]
                        slide = grad[1, 0, 0] - grad[1, 0, 1] + shear
                        rest_out[...] = state[1, VX, 0] - state[1, VY, 0] + earth[0, 0] * slide
                        send_rest.start()

            elif w == 1:

                @pl.when(has_high)
                def _():
                    if not deep:
                        pltpu.make_async_copy(rest_in, rest_in, init_recv.at[6]).wait()
                    send_rest.wait_recv()

                shear = state[1, SXZ, last] - state[1, SYZ, last]
                if deep:
                    slide = grad[1, ABOVE, 0] - grad[1, ABOVE, 1] + (rest_in[...] - shear)
                    gap = above[1, 0] - above[1, 1] + above_earth[0] * slide
                else:
                    hb = above_earth[0] if paired else above_earth[0] * h
                    gap = rest_in[...] - hb * shear
                for p in range(planes):
                    if 0 < p < last - 1:
                        continue
                    vx, vy, vz = (state[1, i, p] for i in (VX, VY, VZ))
                    if p == last:
                        turn = gap - (vx - vy), 0.0
                    else:
                        turn = state[1, VX, p + 1] - vx, state[1, VY, p + 1] - vy
                    curl(1, p, n + 1, *turn, fx(vz), fy(vz))

        for w in range(2):
            load_state[w].wait()
            if w == 1:
                if deep:

                    @pl.when(has_low)
                    def _():
                        down_far[1].start()

                fill(0, 0)
            if deep:
                values, shear, rise = b_fast(w, 0, LOWEST, 0, True, None, None)
                store(down_out, values, w, 0)
                start_down(w, 0, 0)
                down_out[w, 0, 2] = rise(shear(), state[w, SZZ, 1])
                start_down(w, 0, 1)
                set_slope(w, LOWEST, state[w, VZ, 0])
            for p in sorted({0, last}):
                set_grad(w, edge_at(p), *(state[w, i, p] for i in (SXX, SYY, SXY)))
            inside(w, 0)
        lax.fori_loop(1, steps, fill, 0)
        for w in range(2):
            half(w, 0, True, False)

        @pl.when(has_low)
        def _():
            up_earth[1].wait_recv()

        below_earth[1] = below_earth[1] * h

        def take_ghost(w):
            @pl.when(has_high)
            def _():
                down_far[w].wait_recv()

            set_grad(w, ABOVE, above[w, 2], above[w, 3], above[w, 4])

        if deep:

            @pl.when(has_high)
            def _():
                down_earth.wait_recv()

            for i in range(3):
                above_earth[i] = above_earth[i] * h

            @pl.when(has_high)
            def _():
                share_near.start()

            take_ghost(0)
            if steps == 2:
                take_ghost(1)
        elif not paired:

            @pl.when(has_low)
            def _():
                down_near.start()

        def body(n, carry):
            half(0, n, False, False)
            if deep:
                pl.when(n == 1)(lambda: take_ghost(1))
            half(1, n, False, False)
            return carry

        lax.fori_loop(1, steps - 1, body, 0)
        for p in range(1, last - 1):
            vx, vy, vz = (state[1, i, p] for i in (VX, VY, VZ))
            curl(1, p, steps, state[1, VX, p + 1] - vx, state[1, VY, p + 1] - vy, fx(vz), fy(vz))
        if deep:
            for i in early:
                gather_pair(i).start()
        half(0, steps - 1, False, True)
        if not deep:
            merge_pair(early)
        half(1, steps - 1, False, True)
        if deep:
            for i in late:
                gather_pair(i).start()
            arrived(out, sum_recv.at[4], early + late)
            arrived(image, sum_send.at[0], early + late)
        else:
            for i in late:
                merge_pair([i])
            for which in [early] + [[i] for i in late]:
                merge_all(which)
            for k in range(1, pairs):
                arrived(near_sum, sum_send.at[2], early + late)
            if paired:
                arrived(out, sum_send.at[1], early + late)

    if paired:
        pl.when(far)(lambda: run(True))
        pl.when(jnp.logical_not(far))(lambda: run(False))
    else:
        run(False)

    def left(src, sem):
        pltpu.make_async_copy(src, src, sem).wait()

    @pl.when(has_high)
    def _():
        left(below, init_send.at[0])
        left(earth_last, init_send.at[1])
        left(up_out.at[:, pl.ds(0, steps - 1)], step_send.at[0])

    def drain_near():
        if not paired:

            @pl.when(has_low)
            def _():
                down_near.wait_send()

    def drain_far():
        @pl.when(has_low)
        def _():
            left(ghost_down, init_send.at[4])
            down_earth.wait_send()

        @pl.when(has_high)
        def _():
            share_near.wait_send()

    if paired:
        pl.when(far)(drain_far)
        pl.when(jnp.logical_not(far))(drain_near)
    else:
        drain_near()

    @pl.when(has_low)
    def _():
        left(first_down, init_send.at[2])
        send_rest.wait_send()
        left(down_out.at[:, pl.ds(0, steps - 1)], step_send.at[1])


def on_device(
    gz_count,
    shot_count,
    wavefields,
    earth_model,
    source_depth,
    source_column,
    wavelet,
    receiver_depth,
    receiver_column,
    traces,
):
    planes, nx, ny = wavefields.shape[3:]
    steps = wavelet.shape[1]
    rows = 2 * planes * nx
    groups = max((shot_count + 1) // 2 - 1, 1)
    f32 = jnp.float32
    vmem = pl.BlockSpec(memory_space=pltpu.VMEM)
    hbm = pl.BlockSpec(memory_space=pltpu.HBM)
    dma = pltpu.SemaphoreType.DMA

    def plane(*lead):
        return pltpu.VMEM((*lead, nx, ny), f32)

    summed = pl.pallas_call(
        functools.partial(kernel, gz_count, shot_count),
        out_shape=pltpu.VMEM((rows, ny), f32),
        in_specs=[hbm] * 8,
        out_specs=vmem,
        scratch_shapes=[
            plane(2, 9, planes),
            plane(3, planes),
            plane(2, 3),
            plane(2),
            plane(2, 6),
            plane(3),
            plane(2, 4),
            plane(2),
            plane(2, 5),
            plane(2),
            plane(3),
            plane(2, steps, 3),
            plane(2, steps, 3),
            plane(2, steps, 3),
            plane(2, steps, 3),
            plane(),
            plane(),
            plane(steps, planes + 1),
            plane(2, planes),
            plane(planes),
            plane(2, 3, 2),
            plane(2, 3, 2),
            plane(2, 3, 2),
            plane(2),
            pltpu.VMEM((rows, ny), f32),
            pltpu.VMEM((rows, ny), f32),
            pltpu.VMEM((rows, ny), f32),
            pltpu.VMEM((groups, rows, ny), f32),
            pltpu.SMEM(source_depth.shape, jnp.int32),
            pltpu.SMEM(source_column.shape, jnp.int32),
            pltpu.SMEM(wavelet.shape, f32),
            pltpu.VMEM(receiver_depth.shape, jnp.int32),
            pltpu.VMEM(receiver_column.shape, jnp.int32),
            pltpu.VMEM(traces.shape[1:], f32),
            dma((15,)),
            dma((6,)),
            dma((9,)),
            dma((2,)),
            dma((2, 2, 3)),
            dma((2, 2, 3)),
            dma((2,)),
            dma((3,)),
            dma((5,)),
            dma((groups, 4)),
        ],
        compiler_params=pltpu.CompilerParams(collective_id=0, has_side_effects=True),
    )(
        wavefields,
        earth_model,
        source_depth,
        source_column,
        wavelet,
        receiver_depth,
        receiver_column,
        traces,
    )
    return summed.reshape(2, planes, nx, ny)


def solution(mesh):
    placed = (
        P(("parts", "shot"), None, None, "gz", None, None),
        P("parts", "gz", None, None),
        P(("parts", "shot")),
        P(("parts", "shot")),
        P(("parts", "shot"), None),
        P(("parts", "shot"), None),
        P(("parts", "shot"), None),
        P(("parts", "shot"), None, None),
    )
    return jax.shard_map(
        functools.partial(on_device, mesh.shape["gz"], mesh.shape["shot"]),
        mesh=mesh,
        in_specs=placed,
        out_specs=P("parts", "gz", None, None),
        check_vma=False,
    )
```

```python
import functools

import jax
import jax.numpy as jnp
from jax import lax
from jax.experimental import pallas as pl
from jax.experimental.pallas import tpu as pltpu
from jax.sharding import PartitionSpec as P

time_step = 0.15
VX, VY, VZ, SXX, SYY, SZZ, SXY, SXZ, SYZ = range(9)
MESH = pl.DeviceIdType.MESH


def kernel(
    gz_count,
    shot_count,
    wave_hbm,
    earth_hbm,
    src_depth_hbm,
    src_column_hbm,
    wavelet_hbm,
    rec_depth_hbm,
    rec_column_hbm,
    traces_hbm,
    out,
    state,
    earth,
    below,
    below_earth,
    above,
    above_earth,
    first_up,
    first_down,
    ghost_down,
    earth_last,
    earth_first,
    low_in,
    high_in,
    up_out,
    down_out,
    rest_in,
    rest_out,
    inject,
    press,
    spin,
    slope,
    grad,
    strain,
    twist,
    image,
    near_in,
    near_sum,
    cross_in,
    src_depth,
    src_column,
    wavelet,
    rec_depth,
    rec_column,
    traces,
    load_sem,
    init_send,
    init_recv,
    step_send,
    up_recv,
    down_recv,
    rest_sem,
    sum_send,
    sum_recv,
    cross_recv,
):
    planes, nx, ny = state.shape[2:]
    steps = traces.shape[0]
    last = planes - 1
    h = time_step
    gz = lax.axis_index("gz")
    shot = lax.axis_index("shot")
    has_low = gz > 0
    has_high = gz < gz_count - 1
    paired = shot_count % 2 == 0
    far = lax.rem(shot, 2) == 0

    def local(src, dst, k):
        return pltpu.make_async_copy(src, dst, load_sem.at[k])

    def loaded(dst, k):
        local(dst, dst, k).wait()

    load_first = [
        [
            local(wave_hbm.at[0, w, pl.ds(SXZ, 2), last], first_up.at[w, pl.ds(0, 2)], w),
            local(wave_hbm.at[0, w, VZ, last], first_up.at[w, 2], w),
            local(wave_hbm.at[0, w, SZZ, last], first_up.at[w, 3], w),
        ]
        for w in range(2)
    ]
    load_down = local(wave_hbm.at[0, :, SZZ, 0], first_down, 2)
    load_ghost = [
        local(wave_hbm.at[0, :, pl.ds(VX, 2), 0], ghost_down.at[:, pl.ds(0, 2)], 3),
        local(wave_hbm.at[0, :, pl.ds(SXX, 2), 0], ghost_down.at[:, pl.ds(2, 2)], 3),
        local(wave_hbm.at[0, :, SXY, 0], ghost_down.at[:, 4], 3),
    ]
    load_state = [local(wave_hbm.at[0, w], state.at[w], 4 + w) for w in range(2)]
    load_edges = [
        local(earth_hbm.at[0, last], earth_last.at[0], 6),
        local(earth_hbm.at[2, last], earth_last.at[1], 6),
    ]
    load_lowest = local(earth_hbm.at[:, 0], earth_first, 7)
    load_earth = local(earth_hbm, earth, 8)
    small = [
        local(src, dst, 9 + i)
        for i, (src, dst) in enumerate(
            (
                (traces_hbm.at[0], traces),
                (rec_depth_hbm, rec_depth),
                (rec_column_hbm, rec_column),
                (src_depth_hbm, src_depth),
                (src_column_hbm, src_column),
                (wavelet_hbm, wavelet),
            )
        )
    ]
    for copy in load_edges + load_first[0] + [load_down] + load_first[1]:
        copy.start()
    for copy in load_ghost + [load_lowest, load_state[0], load_earth] + small + [load_state[1]]:
        copy.start()

    barrier = pltpu.get_barrier_semaphore()

    @pl.when(has_low)
    def _():
        pl.semaphore_signal(barrier, inc=1, device_id={"gz": gz - 1}, device_id_type=MESH)

    @pl.when(has_high)
    def _():
        pl.semaphore_signal(barrier, inc=1, device_id={"gz": gz + 1}, device_id_type=MESH)

    for k in range(1, shot_count):
        peer = lax.rem(shot + k, shot_count)
        pl.semaphore_signal(barrier, inc=1, device_id={"shot": peer}, device_id_type=MESH)

    rows = lax.broadcasted_iota(jnp.int32, (nx, ny), 0)
    lanes = lax.broadcasted_iota(jnp.int32, (nx, ny), 1)
    cells = rows * ny + lanes

    def fx(a):
        return jnp.where(rows == nx - 1, 0.0, pltpu.roll(a, nx - 1, 0)) - a

    def bx(a):
        return a - jnp.where(rows == 0, 0.0, pltpu.roll(a, 1, 0))

    def fy(a):
        return jnp.where(lanes == ny - 1, 0.0, pltpu.roll(a, ny - 1, 1)) - a

    def by(a):
        return a - jnp.where(lanes == 0, 0.0, pltpu.roll(a, 1, 1))

    low_peers = (gz + gz_count - 1) // gz_count
    high_peers = (2 * gz_count - 2 - gz) // gz_count
    pl.semaphore_wait(barrier, low_peers + high_peers + shot_count - 1)

    def remote(src, dst, send, recv, step_to):
        return pltpu.make_async_remote_copy(
            src_ref=src,
            dst_ref=dst,
            send_sem=send,
            recv_sem=recv,
            device_id={"gz": gz + step_to},
            device_id_type=MESH,
        )

    def initial(src, dst, k, m, step_to):
        return remote(src, dst, init_send.at[m], init_recv.at[k], step_to)

    up_first = [initial(first_up.at[w, pl.ds(0, 3)], below.at[w], w, 0, 1) for w in range(2)]
    up_earth = [initial(earth_last.at[k], below_earth.at[k], 2 + k, 1, 1) for k in range(2)]
    down_first = [initial(first_down.at[w], above.at[w, 5], 4 + w, 2, -1) for w in range(2)]
    if paired:
        share_near = pltpu.make_async_remote_copy(
            src_ref=above_earth.at[0],
            dst_ref=above_earth.at[0],
            send_sem=init_send.at[5],
            recv_sem=init_recv.at[6],
            device_id={"shot": shot + 1},
            device_id_type=MESH,
        )
    else:
        down_near = initial(earth_first.at[0], above_earth.at[0], 6, 3, -1)
    down_earth = initial(earth_first, above_earth, 6, 3, -1)
    down_far = [initial(ghost_down.at[w], above.at[w, pl.ds(0, 5)], 7 + w, 4, -1) for w in range(2)]

    loaded(earth_last, 6)
    for w in range(2):
        loaded(first_up.at[w], w)
        around = bx(first_up[w, 0]) + by(first_up[w, 1]) - first_up[w, 3]
        first_up[w, 2] = first_up[w, 2] + (h * earth_last[0]) * around

        @pl.when(has_high)
        def _(w=w):
            up_first[w].start()
            up_earth[w].start()

        if w == 0:
            load_down.wait()

        @pl.when(has_low)
        def _(w=w):
            down_first[w].start()

    load_lowest.wait()
    loaded(ghost_down, 3)

    if paired:

        @pl.when(has_low & far)
        def _():
            down_far[0].start()
            down_earth.start()

    @pl.when(jnp.logical_not(has_low))
    def _():
        below[...] = jnp.zeros_like(below)
        below_earth[...] = jnp.zeros_like(below_earth)
        low_in[...] = jnp.zeros_like(low_in)

    @pl.when(jnp.logical_not(has_high))
    def _():
        above[...] = jnp.zeros_like(above)
        above_earth[...] = jnp.zeros_like(above_earth)
        high_in[...] = jnp.zeros_like(high_in)
        rest_in[...] = jnp.zeros_like(rest_in)

    image[...] = jnp.zeros_like(image)
    load_earth.wait()
    earth[...] = earth[...] * h

    offset = gz * planes
    for copy in small:
        copy.wait()
    receivers = traces.shape[1]
    column = rec_column[...]
    depth = rec_depth[...] - offset
    row_ids = lax.broadcasted_iota(jnp.int32, (nx, receivers), 0) * ny
    past = column - row_ids
    on_row = (past >= 0) & (past < ny)
    row_hot = jnp.concatenate(
        [jnp.where(on_row & (depth == p), h, 0.0) for p in range(-1, planes)], axis=0
    )
    col_ids = lax.broadcasted_iota(jnp.int32, (ny, receivers), 0)
    col_hot = jnp.where((column & (ny - 1)) == col_ids, 1.0, 0.0)

    def fill(n, carry):
        inject[n] = lax.dot_general(
            row_hot * traces[pl.ds(n, 1), :],
            col_hot,
            (((1,), (1,)), ((), ())),
            precision=lax.Precision.HIGHEST,
            preferred_element_type=jnp.float32,
        ).reshape(planes + 1, nx, ny)
        return carry

    src_at = src_depth[0] - offset
    src_cell = src_column[0]

    def source_term(plane, n):
        cell = jnp.where(src_at == plane, src_cell, -1)
        return jnp.where(cells == cell, h * wavelet[0, n], 0.0)

    def parity(n):
        return n % 2 if isinstance(n, int) else lax.rem(n, 2)

    def mod3(n):
        return n % 3 if isinstance(n, int) else lax.rem(n, 3)

    def part_of(ref, w, n, part):
        return ref.at[w, n, pl.ds(0, 2)] if part == 0 else ref.at[w, n, 2]

    def send_up(w, n, part):
        return remote(
            part_of(up_out, w, n, part),
            part_of(low_in, w, n, part),
            step_send.at[0],
            up_recv.at[w, part, mod3(n)],
            1,
        )

    def send_down(w, n, part):
        return remote(
            part_of(down_out, w, n, part),
            part_of(high_in, w, n, part),
            step_send.at[1],
            down_recv.at[w, part, mod3(n)],
            -1,
        )

    send_rest = remote(rest_out, rest_in, rest_sem.at[0], rest_sem.at[1], -1)

    def strains(w, p, n, vx, vy, dvz, hlam, hmu):
        ex, ey = bx(vx), by(vy)
        spread = hlam * (ex + ey + dvz)
        if w == 0:
            spread = spread + source_term(p, n)
        mu2 = 2.0 * hmu
        return spread + mu2 * ex, spread + mu2 * ey, spread + mu2 * dvz

    def keep_pressure(w, p, n, total):
        at = parity(n + 1)
        if w == 0:
            press[at, p] = total * (1.0 / (3 * steps))
        else:
            image[pl.ds(p * nx, nx), :] += press[at, p] * (total * (1.0 / 3.0))

    def a_node(w, p, n):
        hb, hlam, hmu = (earth[i, p] for i in range(3))
        sxy = state[w, SXY, p]
        below_p = (below[w, i] for i in range(3)) if p == 0 else (state[w, i, p - 1] for i in (SXZ, SYZ, VZ))
        sxz_b, syz_b, vz_b = below_p
        vx = state[w, VX, p] + hb * (fx(state[w, SXX, p]) + by(sxy) + (state[w, SXZ, p] - sxz_b))
        vy = state[w, VY, p] + hb * (bx(sxy) + fy(state[w, SYY, p]) + (state[w, SYZ, p] - syz_b))
        state[w, VX, p] = vx
        state[w, VY, p] = vy
        dxx, dyy, dzz = strains(w, p, n, vx, vy, state[w, VZ, p] - vz_b, hlam, hmu)
        sxx = state[w, SXX, p] + dxx
        syy = state[w, SYY, p] + dyy
        szz = state[w, SZZ, p] + dzz
        total = sxx + syy + szz
        state[w, SXX, p] = sxx
        state[w, SYY, p] = syy
        state[w, SZZ, p] = szz
        vxy, vyx = fy(vx), fx(vy)
        state[w, SXY, p] = sxy + hmu * (vxy + vyx)
        keep_pressure(w, p, n, total)
        if w == 1:
            spin[p] = vyx - vxy

    def curl(w, p, n, vxz, vyz, vzx, vzy):
        rotation = (vzy - vyz) + (vxz - vzx) + spin[p]
        image[pl.ds((planes + p) * nx, nx), :] += press[parity(n), p] * rotation

    def b_node(w, p, n, first, upper):
        hb, hmu = earth[0, p], earth[2, p]
        vz, sxz, syz = (state[w, i, p] for i in (VZ, SXZ, SYZ))
        vx_f, vy_f, szz_f = upper
        if not first:
            vxz, vyz = vx_f - state[w, VX, p], vy_f - state[w, VY, p]
            vzx, vzy = fx(vz), fy(vz)
            sxz = sxz + hmu * (vxz + vzx)
            syz = syz + hmu * (vyz + vzy)
            state[w, SXZ, p] = sxz
            state[w, SYZ, p] = syz
            if w == 1:
                curl(w, p, n, vxz, vyz, vzx, vzy)
        term = hb * (bx(sxz) + by(syz) + (szz_f - state[w, SZZ, p]))
        if w == 1:
            term = term + inject[n, p + 1]
        vz = vz + term
        state[w, VZ, p] = vz
        return sxz, syz, vz

    def own_upper(w, p):
        return tuple(state[w, i, p + 1] for i in (VX, VY, SZZ))

    BELOW, LAST, LOWEST = range(3)
    ABOVE = 2

    def edge_at(p):
        return 0 if p == 0 else 1

    def set_slope(w, slot, vz):
        slope[w, slot, 0] = fx(vz)
        slope[w, slot, 1] = fy(vz)

    def set_grad(w, slot, sxx, syy, sxy):
        grad[w, slot, 0] = fx(sxx) + by(sxy)
        grad[w, slot, 1] = bx(sxy) + fy(syy)

    def edge_velocity(w, p):
        hb = earth[0, p]
        if p == 0:
            sxz_b, syz_b = below[w, 0], below[w, 1]
        else:
            sxz_b, syz_b = state[w, SXZ, p - 1], state[w, SYZ, p - 1]
        at = edge_at(p)
        vx = state[w, VX, p] + hb * (grad[w, at, 0] + (state[w, SXZ, p] - sxz_b))
        vy = state[w, VY, p] + hb * (grad[w, at, 1] + (state[w, SYZ, p] - syz_b))
        return vx, vy

    def edge_rise(w, p):
        return state[w, VZ, p] - (below[w, 2] if p == 0 else state[w, VZ, p - 1])

    def widen(w, at, p, n, vx, vy, hlam, hmu):
        ey = by(vy)
        strain[w, at, 1] = ey
        flat = bx(vx) + ey

        def finish(dvz):
            spread = hlam * (flat + dvz)
            if w == 0:
                spread = spread + source_term(p, n)
            strain[w, at, 0] = spread
            return spread + (2.0 * hmu) * dvz

        return finish

    def a_fast(w, p, n):
        vx, vy = edge_velocity(w, p)
        state[w, VX, p] = vx
        state[w, VY, p] = vy
        change = widen(w, edge_at(p), p, n, vx, vy, earth[1, p], earth[2, p])

        def finish():
            szz = state[w, SZZ, p] + change(edge_rise(w, p))
            state[w, SZZ, p] = szz
            return szz

        return (vx, vy), finish

    def rest_of(w, at, vx, vy, hmu, sxx, syy, sxy):
        spread, mu2 = strain[w, at, 0], 2.0 * hmu
        vxy, vyx = fy(vx), fx(vy)
        sxx = sxx + (spread + mu2 * bx(vx))
        syy = syy + (spread + mu2 * strain[w, at, 1])
        sxy = sxy + hmu * (vxy + vyx)
        set_grad(w, at, sxx, syy, sxy)
        return sxx, syy, sxy, vyx - vxy

    def a_slow(w, p, n):
        sxx, syy, sxy, turn = rest_of(
            w, edge_at(p), *(state[w, i, p] for i in (VX, VY)), earth[2, p],
            *(state[w, i, p] for i in (SXX, SYY, SXY)),
        )
        state[w, SXX, p] = sxx
        state[w, SYY, p] = syy
        state[w, SXY, p] = sxy
        keep_pressure(w, p, n, sxx + syy + state[w, SZZ, p])
        if w == 1:
            spin[p] = turn

    def a_final(w, p, n):
        vx, vy = edge_velocity(w, p)
        volume = bx(vx) + by(vy) + edge_rise(w, p)
        spread = earth[1, p] * volume
        if w == 0:
            spread = spread + source_term(p, n)
        total = state[w, SXX, p] + state[w, SYY, p] + state[w, SZZ, p]
        keep_pressure(w, p, n, total + (3.0 * spread + (2.0 * earth[2, p]) * volume))
        if w == 1:
            state[1, VX, p] = vx
            state[1, VY, p] = vy
            spin[p] = fx(vy) - fy(vx)

    def b_fast(w, p, slot, n, first, vx_f, vy_f):
        sxz, syz = state[w, SXZ, p], state[w, SYZ, p]
        if not first:
            hmu = earth[2, p]
            vxz, vyz = vx_f - state[w, VX, p], vy_f - state[w, VY, p]
            vzx, vzy = slope[w, slot, 0], slope[w, slot, 1]
            sxz = sxz + hmu * (vxz + vzx)
            syz = syz + hmu * (vyz + vzy)
            state[w, SXZ, p] = sxz
            state[w, SYZ, p] = syz
            if w == 1:
                twist[edge_at(p)] = (vzy - vyz) + (vxz - vzx)

        def flat():
            return bx(sxz) + by(syz)

        def finish(shear, szz_f):
            term = earth[0, p] * (shear + (szz_f - state[w, SZZ, p]))
            if w == 1:
                term = term + inject[n, p + 1]
            vz = state[w, VZ, p] + term
            state[w, VZ, p] = vz
            return vz

        return (sxz, syz), flat, finish

    def keep_twist(p, n):
        image[pl.ds((planes + p) * nx, nx), :] += press[parity(n), p] * (
            twist[edge_at(p)] + spin[p]
        )

    def b_below(w, n, first):
        if not first:
            hmu = below_earth[1]
            vx_m, vy_m = low_in[w, n - 1, 0], low_in[w, n - 1, 1]
            sxz = below[w, 0] + hmu * ((state[w, VX, 0] - vx_m) + slope[w, BELOW, 0])
            syz = below[w, 1] + hmu * ((state[w, VY, 0] - vy_m) + slope[w, BELOW, 1])
            below[w, 0] = sxz
            below[w, 1] = syz

        def flat():
            return None if first else bx(sxz) + by(syz)

        def finish(shear):
            szz = state[w, SZZ, 0]
            term = below_earth[0] * (szz if first else shear + (szz - low_in[w, n - 1, 2]))
            if w == 1:
                term = term + inject[n, 0]
            below[w, 2] = below[w, 2] + term

        return flat, finish

    def above_velocity(w, sxz, syz):
        hb = above_earth[0]
        vx = above[w, 0] + hb * (grad[w, ABOVE, 0] + (sxz - state[w, SXZ, last]))
        vy = above[w, 1] + hb * (grad[w, ABOVE, 1] + (syz - state[w, SYZ, last]))
        return vx, vy

    def above_fast(w, n):
        vx, vy = above_velocity(w, high_in[w, n - 1, 0], high_in[w, n - 1, 1])
        above[w, 0] = vx
        above[w, 1] = vy
        change = widen(w, ABOVE, planes, n - 1, vx, vy, above_earth[1], above_earth[2])

        def finish():
            szz = above[w, 5] + change(high_in[w, n - 1, 2] - state[w, VZ, last])
            above[w, 5] = szz
            return szz

        return (vx, vy), finish

    def above_slow(w):
        sxx, syy, sxy, _ = rest_of(
            w, ABOVE, above[w, 0], above[w, 1], above_earth[2], above[w, 2], above[w, 3], above[w, 4]
        )
        above[w, 2] = sxx
        above[w, 3] = syy
        above[w, 4] = sxy

    def left(src, sem):
        pltpu.make_async_copy(src, src, sem).wait()

    def drain_near():
        if not paired:

            @pl.when(has_low)
            def _():
                down_near.wait_send()

    def drain_far():
        @pl.when(has_low)
        def _():
            left(ghost_down, init_send.at[4])
            down_earth.wait_send()

        @pl.when(has_high)
        def _():
            share_near.wait_send()

    def drain(deep):
        @pl.when(has_high)
        def _():
            left(below, init_send.at[0])
            left(earth_last, init_send.at[1])
            left(up_out.at[:, pl.ds(0, steps - 1)], step_send.at[0])

        drain_far() if deep else drain_near()

        @pl.when(has_low)
        def _():
            left(first_down, init_send.at[2])
            send_rest.wait_send()
            left(down_out.at[:, pl.ds(0, steps - 1)], step_send.at[1])

    inner = range(1, last)
    bounds = [(nx, last * nx), ((planes + 1) * nx, (planes + last - 1) * nx)]
    early = [i for i in range(2) if bounds[i][1] > bounds[i][0]]
    bounds += [(0, nx), (last * nx, (planes + 1) * nx), ((planes + last - 1) * nx, 2 * planes * nx)]
    late = [2, 3, 4]
    pairs = shot_count // 2 if paired else shot_count

    def piece(i):
        return pl.ds(bounds[i][0], bounds[i][1] - bounds[i][0])

    def to_shot(src, dst, send, recv, target):
        return pltpu.make_async_remote_copy(
            src_ref=src,
            dst_ref=dst,
            send_sem=send,
            recv_sem=recv,
            device_id={"shot": target},
            device_id_type=MESH,
        )

    def group(i):
        return 0 if i in early else i - 1

    def gather_pair(i):
        sems = sum_send.at[0], sum_recv.at[group(i)]
        return to_shot(image.at[piece(i)], near_in.at[piece(i)], *sems, shot + 1)

    def give_back(i):
        sems = sum_send.at[1], sum_recv.at[4]
        return to_shot(out.at[piece(i)], out.at[piece(i)], *sems, shot - 1)

    def cross(i, k):
        target = lax.rem(shot + k * (shot_count // pairs), shot_count)
        sems = sum_send.at[2], cross_recv.at[k - 1, group(i)]
        return to_shot(near_sum.at[piece(i)], cross_in.at[k - 1, piece(i)], *sems, target)

    def arrived(dst, sem, which):
        count = sum(bounds[i][1] - bounds[i][0] for i in which)
        whole = dst.at[pl.ds(0, count)]
        pltpu.make_async_copy(whole, whole, sem).wait()

    def merge_pair(which):
        if paired:
            arrived(near_in, sum_recv.at[group(which[0])], which)
        for i in which:
            near_sum[piece(i), :] = image[piece(i), :]
            if paired:
                near_sum[piece(i), :] += near_in[piece(i), :]
            for k in range(1, pairs):
                cross(i, k).start()

    def merge_all(which):
        for k in range(1, pairs):
            arrived(cross_in.at[k - 1], cross_recv.at[k - 1, group(which[0])], which)
        for i in which:
            total = near_sum[piece(i), :]
            for k in range(1, pairs):
                total = total + cross_in[k - 1, piece(i), :]
            out[piece(i), :] = total
            if paired:
                give_back(i).start()

    def run(deep):
        def inside(w, n):
            for p in range(1 if deep else 0, last):
                b_node(w, p, n, isinstance(n, int) and n == 0, own_upper(w, p))
            for p in inner:
                a_node(w, p, n)

        def store(buf, values, w, n):
            for i, value in enumerate(values):
                buf[w, n, i] = value

        def start_up(w, n, part):
            @pl.when(has_high)
            def _():
                send_up(w, n, part).start()

        def start_down(w, n, part):
            @pl.when((has_low & (n < steps - 1)) if deep else has_low)
            def _():
                send_down(w, n, part).start()

        def wait_high(w, n, part):
            @pl.when(has_high)
            def _():
                send_down(w, n, part).wait_recv()

        def wait_low(w, n, part):
            @pl.when(has_low)
            def _():
                send_up(w, n, part).wait_recv()

        def first_low(w):
            @pl.when(has_low)
            def _():
                up_first[w].wait_recv()
                if w == 0:
                    up_earth[0].wait_recv()

            if w == 0:
                below_earth[0] = below_earth[0] * h

        def half(w, n, first, final):
            if first:

                @pl.when(has_high)
                def _():
                    down_first[w].wait_recv()

                szz_f = above[w, 5]
            vx_f = vy_f = None
            if final:
                for part in range(2):
                    wait_high(w, n - 1, part)
                    wait_low(w, n - 1, part)
                if deep:
                    (vx_f, vy_f), lift = above_fast(w, n)
                    szz_f = lift()
                else:
                    vx_f, vy_f, szz_f = (high_in[w, n - 1, i] for i in range(3))
                _, shear, rise = b_fast(w, last, LAST, n, first, vx_f, vy_f)
                rise(shear(), szz_f)
                shear, rise = b_below(w, n, first)
                rise(shear())
                if w == 1:
                    keep_twist(last, n)
                    if deep:
                        above_slow(w)
                a_final(w, 0, n)
                a_final(w, last, n)
            elif deep:
                if not first:
                    wait_high(w, n - 1, 0)
                    (vx_f, vy_f), lift = above_fast(w, n)
                _, shear, rise = b_fast(w, last, LAST, n, first, vx_f, vy_f)
                values, top = a_fast(w, last, n)
                store(up_out, values, w, n)
                start_up(w, n, 0)
                shear = shear()
                if not first:
                    wait_high(w, n - 1, 1)
                    szz_f = lift()
                rise(shear, szz_f)
                up_out[w, n, 2] = top()
                start_up(w, n, 1)
                if first:
                    first_low(w)
                else:
                    wait_low(w, n - 1, 0)
                shear_m, rise_m = b_below(w, n, first)
                _, bottom = a_fast(w, 0, n)
                lower = (state[w, VX, 1], state[w, VY, 1])
                values, shear, rise = b_fast(w, 0, LOWEST, n + 1, False, *lower)
                store(down_out, values, w, n + 1)
                if w == 1:

                    @pl.when(has_low & (n == steps - 2))
                    def _():
                        rest_out[...] = state[1, SXZ, 0] - state[1, SYZ, 0]
                        send_rest.start()

                start_down(w, n + 1, 0)
                shear_m, shear = shear_m(), shear()
                if not first:
                    wait_low(w, n - 1, 1)
                rise_m(shear_m)
                bottom()
                down_out[w, n + 1, 2] = rise(shear, state[w, SZZ, 1])
                start_down(w, n + 1, 1)
            else:
                if first:
                    first_low(w)
                else:
                    wait_low(w, n - 1, 0)
                    wait_high(w, n - 1, 0)
                    vx_f, vy_f = high_in[w, n - 1, 0], high_in[w, n - 1, 1]
                shear_m, rise_m = b_below(w, n, first)
                _, shear, rise = b_fast(w, last, LAST, n, first, vx_f, vy_f)
                values, bottom = a_fast(w, 0, n)
                store(down_out, values, w, n)
                values, top = a_fast(w, last, n)
                store(up_out, values, w, n)
                start_down(w, n, 0)
                start_up(w, n, 0)
                shear_m, shear = shear_m(), shear()
                if not first:
                    wait_low(w, n - 1, 1)
                    wait_high(w, n - 1, 1)
                    szz_f = high_in[w, n - 1, 2]
                rise_m(shear_m)
                rise(shear, szz_f)
                down_out[w, n, 2] = bottom()
                up_out[w, n, 2] = top()
                start_down(w, n, 1)
                start_up(w, n, 1)

            if not final:
                if w == 1 and not first:
                    keep_twist(last, n)
                a_slow(w, 0, n)
                a_slow(w, last, n)
                if deep:
                    if not first:
                        above_slow(w)
                    if w == 1:
                        keep_twist(0, n + 1)
                    set_slope(w, LOWEST, state[w, VZ, 0])
                set_slope(w, BELOW, below[w, 2])
                set_slope(w, LAST, state[w, VZ, last])
                inside(w, n + 1)
                if w == 1 and not deep:

                    @pl.when(has_low & (n == steps - 2))
                    def _():
                        shear = state[1, SXZ, 0] - state[1, SYZ, 0]
                        slide = grad[1, 0, 0] - grad[1, 0, 1] + shear
                        rest_out[...] = state[1, VX, 0] - state[1, VY, 0] + earth[0, 0] * slide
                        send_rest.start()

            elif w == 1:

                @pl.when(has_high)
                def _():
                    if not deep:
                        pltpu.make_async_copy(rest_in, rest_in, init_recv.at[6]).wait()
                    send_rest.wait_recv()

                shear = state[1, SXZ, last] - state[1, SYZ, last]
                if deep:
                    slide = grad[1, ABOVE, 0] - grad[1, ABOVE, 1] + (rest_in[...] - shear)
                    gap = above[1, 0] - above[1, 1] + above_earth[0] * slide
                else:
                    hb = above_earth[0] if paired else above_earth[0] * h
                    gap = rest_in[...] - hb * shear
                for p in range(planes):
                    if 0 < p < last - 1:
                        continue
                    vx, vy, vz = (state[1, i, p] for i in (VX, VY, VZ))
                    if p == last:
                        turn = gap - (vx - vy), 0.0
                    else:
                        turn = state[1, VX, p + 1] - vx, state[1, VY, p + 1] - vy
                    curl(1, p, n + 1, *turn, fx(vz), fy(vz))

        for w in range(2):
            load_state[w].wait()
            if w == 1:
                if deep:

                    @pl.when(has_low)
                    def _():
                        down_far[1].start()

                fill(0, 0)
            if deep:
                values, shear, rise = b_fast(w, 0, LOWEST, 0, True, None, None)
                store(down_out, values, w, 0)
                start_down(w, 0, 0)
                down_out[w, 0, 2] = rise(shear(), state[w, SZZ, 1])
                start_down(w, 0, 1)
                set_slope(w, LOWEST, state[w, VZ, 0])
            for p in sorted({0, last}):
                set_grad(w, edge_at(p), *(state[w, i, p] for i in (SXX, SYY, SXY)))
            inside(w, 0)
        lax.fori_loop(1, steps, fill, 0)
        for w in range(2):
            half(w, 0, True, False)

        @pl.when(has_low)
        def _():
            up_earth[1].wait_recv()

        below_earth[1] = below_earth[1] * h

        def take_ghost(w):
            @pl.when(has_high)
            def _():
                down_far[w].wait_recv()

            set_grad(w, ABOVE, above[w, 2], above[w, 3], above[w, 4])

        if deep:

            @pl.when(has_high)
            def _():
                down_earth.wait_recv()

            for i in range(3):
                above_earth[i] = above_earth[i] * h

            @pl.when(has_high)
            def _():
                share_near.start()

            take_ghost(0)
            if steps == 2:
                take_ghost(1)
        elif not paired:

            @pl.when(has_low)
            def _():
                down_near.start()

        def body(n, carry):
            half(0, n, False, False)
            if deep:
                pl.when(n == 1)(lambda: take_ghost(1))
            half(1, n, False, False)
            return carry

        lax.fori_loop(1, steps - 1, body, 0)
        for p in range(1, last - 1):
            vx, vy, vz = (state[1, i, p] for i in (VX, VY, VZ))
            curl(1, p, steps, state[1, VX, p + 1] - vx, state[1, VY, p + 1] - vy, fx(vz), fy(vz))
        if deep:
            for i in early:
                gather_pair(i).start()
        half(0, steps - 1, False, True)
        if not deep:
            merge_pair(early)
        half(1, steps - 1, False, True)
        if deep:
            for i in late:
                gather_pair(i).start()
            drain(True)
            arrived(out, sum_recv.at[4], early + late)
            arrived(image, sum_send.at[0], early + late)
        else:
            drain(False)
            for i in late:
                merge_pair([i])
            for which in [early] + [[i] for i in late]:
                merge_all(which)
            for k in range(1, pairs):
                arrived(near_sum, sum_send.at[2], early + late)
            if paired:
                arrived(out, sum_send.at[1], early + late)

    if paired:
        pl.when(far)(lambda: run(True))
        pl.when(jnp.logical_not(far))(lambda: run(False))
    else:
        run(False)


def on_device(
    gz_count,
    shot_count,
    wavefields,
    earth_model,
    source_depth,
    source_column,
    wavelet,
    receiver_depth,
    receiver_column,
    traces,
):
    planes, nx, ny = wavefields.shape[3:]
    steps = wavelet.shape[1]
    rows = 2 * planes * nx
    groups = max((shot_count + 1) // 2 - 1, 1)
    f32 = jnp.float32
    vmem = pl.BlockSpec(memory_space=pltpu.VMEM)
    hbm = pl.BlockSpec(memory_space=pltpu.HBM)
    dma = pltpu.SemaphoreType.DMA

    def plane(*lead):
        return pltpu.VMEM((*lead, nx, ny), f32)

    summed = pl.pallas_call(
        functools.partial(kernel, gz_count, shot_count),
        out_shape=pltpu.VMEM((rows, ny), f32),
        in_specs=[hbm] * 8,
        out_specs=vmem,
        scratch_shapes=[
            plane(2, 9, planes),
            plane(3, planes),
            plane(2, 3),
            plane(2),
            plane(2, 6),
            plane(3),
            plane(2, 4),
            plane(2),
            plane(2, 5),
            plane(2),
            plane(3),
            plane(2, steps, 3),
            plane(2, steps, 3),
            plane(2, steps, 3),
            plane(2, steps, 3),
            plane(),
            plane(),
            plane(steps, planes + 1),
            plane(2, planes),
            plane(planes),
            plane(2, 3, 2),
            plane(2, 3, 2),
            plane(2, 3, 2),
            plane(2),
            pltpu.VMEM((rows, ny), f32),
            pltpu.VMEM((rows, ny), f32),
            pltpu.VMEM((rows, ny), f32),
            pltpu.VMEM((groups, rows, ny), f32),
            pltpu.SMEM(source_depth.shape, jnp.int32),
            pltpu.SMEM(source_column.shape, jnp.int32),
            pltpu.SMEM(wavelet.shape, f32),
            pltpu.VMEM(receiver_depth.shape, jnp.int32),
            pltpu.VMEM(receiver_column.shape, jnp.int32),
            pltpu.VMEM(traces.shape[1:], f32),
            dma((15,)),
            dma((6,)),
            dma((9,)),
            dma((2,)),
            dma((2, 2, 3)),
            dma((2, 2, 3)),
            dma((2,)),
            dma((3,)),
            dma((5,)),
            dma((groups, 4)),
        ],
        compiler_params=pltpu.CompilerParams(collective_id=0, has_side_effects=True),
    )(
        wavefields,
        earth_model,
        source_depth,
        source_column,
        wavelet,
        receiver_depth,
        receiver_column,
        traces,
    )
    return summed.reshape(2, planes, nx, ny)


def solution(mesh):
    placed = (
        P(("parts", "shot"), None, None, "gz", None, None),
        P("parts", "gz", None, None),
        P(("parts", "shot")),
        P(("parts", "shot")),
        P(("parts", "shot"), None),
        P(("parts", "shot"), None),
        P(("parts", "shot"), None),
        P(("parts", "shot"), None, None),
    )
    return jax.shard_map(
        functools.partial(on_device, mesh.shape["gz"], mesh.shape["shot"]),
        mesh=mesh,
        in_specs=placed,
        out_specs=P("parts", "gz", None, None),
        check_vma=False,
    )
```
